256 devices in a mesh: gx: 16 (over z, core), gy: 4 (over x), gz: 4 (over y).
Axes of the slice: x: 4, y: 4, z: 8, core: 2. Of those that a mesh axis runs over, the one named last changes fastest.
Arguments:
- block_values: bfloat16 [4, 64, 4, 6, 128, 128], P('gy', 'gx', 'gz'), as said below
- block_cols: int32 [4, 64, 4, 6], P('gy', 'gx', 'gz'), may hold values from 0 to 63, as said below
Outputs:
- purified: float32 [2048, 32768], P(('gx', 'gy'), 'gz')
The draws below stay inside these ranges and needn't reach their ends.
Inputs may be any that keep to these rules, and one draw needn't show every extreme that they name: block_cols[a, s, b, :] holds 6 distinct tile columns of panel b at which tile row a * 64 + s of P is nonzero; every tile column of a panel is listed by exactly 6 tile rows of each slab; the pattern is symmetric: tile (i, j) is listed exactly when tile (j, i) is. `block_values`: P is symmetric: the tile listed at (i, j) is the transpose of the tile listed at (j, i), and diagonal tiles are symmetric.
All inputs are finite; a program needn't handle non-finite values.
Results may differ from the reference program's by a relative error of at most 0.0033.
Values may be sent and summed in bfloat16 or wider, within the bound.
A program may use at most 128 MiB of HBM per device.

```python
import jax
import jax.numpy as jnp
from jax import lax

TILE = 128
NT = 256
KP = 6
WIN = 1
NPAN = 4
ST = 64
RB = 4
ORDER = 32768
N_GX = 16


def tile_pattern(key):
    pattern_key = jax.random.fold_in(key, 11)
    split_keys = jax.random.split(pattern_key, 2)
    order_keys = jax.random.split(split_keys[0], NPAN * NPAN * 2)
    orders = jax.vmap(lambda subkey: jax.random.permutation(subkey, ST))(order_keys).reshape(NPAN, NPAN, 2, ST)
    first = orders[:, :, 0].astype(jnp.int32)
    second = orders[:, :, 1].astype(jnp.int32)
    slab_index = jnp.arange(NPAN, dtype=jnp.int32)[:, None, None]
    panel_index = jnp.arange(NPAN, dtype=jnp.int32)[None, :, None]
    lower_part = slab_index > panel_index
    on_diagonal = slab_index == panel_index
    first_swapped = jnp.swapaxes(first, 0, 1)
    second_swapped = jnp.swapaxes(second, 0, 1)
    source_order = jnp.where(lower_part, second_swapped, first)
    target_order = jnp.where(lower_part, first_swapped, jnp.where(on_diagonal, first, second))
    target_inverse = jnp.argsort(target_order, axis=-1).astype(jnp.int32)
    extra_shifts = (jax.random.permutation(split_keys[1], ST // 2 - 1)[:(KP - 2) // 2] + 1).astype(jnp.int32)
    shifts = jnp.concatenate([jnp.array([0, ST // 2], jnp.int32), extra_shifts, -extra_shifts])
    position = (source_order[:, :, :, None] + shifts[None, None, None, :]) % ST
    columns = jnp.take_along_axis(target_inverse, position.reshape(NPAN, NPAN, ST * KP), axis=2)
    return jnp.transpose(columns.reshape(NPAN, NPAN, ST, KP), (0, 2, 1, 3)).astype(jnp.int32)


def draw_block_cols(key, part):
    return tile_pattern(key)


def draw_block_values(key, part):
    columns = tile_pattern(key)
    row_global = jnp.broadcast_to((jnp.arange(NPAN, dtype=jnp.int32)[:, None] * ST + jnp.arange(ST, dtype=jnp.int32)[None, :])[:, :, None, None], (NPAN, ST, NPAN, KP))
    col_global = jnp.arange(NPAN, dtype=jnp.int32)[None, None, :, None] * ST + columns
    tile_ident = (jnp.minimum(row_global, col_global) * NT + jnp.maximum(row_global, col_global)).reshape(-1)
    value_key = jax.random.fold_in(key, 23)

    def one_tile(ident):
        subkey = jax.random.fold_in(value_key, ident)
        return jax.random.normal(subkey, (TILE, TILE), jnp.float32)
    raw_tiles = jax.vmap(one_tile)(tile_ident)
    flipped = (row_global > col_global).reshape(-1)[:, None, None]
    diagonal_mask = (row_global == col_global).reshape(-1)[:, None, None]
    swapped = jnp.swapaxes(raw_tiles, 1, 2)
    tiles = jnp.where(flipped, swapped, raw_tiles)
    tiles = jnp.where(diagonal_mask, (raw_tiles + swapped) * 0.7071, tiles)
    scale = 2.0 / (NPAN * KP * TILE) ** 0.5
    return (tiles * scale).reshape(NPAN, ST, NPAN, KP, TILE, TILE).astype(jnp.bfloat16)


def setup_inputs(seed: int = 0) -> dict:
    splits = jax.random.split(jax.random.key(seed), 3)
    return {
        "block_values": draw_block_values(jax.random.fold_in(splits[2], 71), 0),
        "block_cols": draw_block_cols(jax.random.fold_in(splits[2], 71), 0),
    }


def dense_rows(row_tiles, row_columns):
    count_rows = row_tiles.shape[0]
    global_cols = (jnp.arange(NPAN, dtype=jnp.int32)[None, :, None] * ST + row_columns).reshape(count_rows, NPAN * KP)
    onehot = (global_cols[:, :, None] == jnp.arange(NT, dtype=jnp.int32)[None, None, :]).astype(jnp.float32)
    flattened = row_tiles.reshape(count_rows, NPAN * KP, TILE, TILE).astype(jnp.float32)
    densified = jnp.einsum("nqj,nqyx->nyjx", onehot, flattened)
    return densified.reshape(count_rows * TILE, ORDER)


def times_matrix(left_rows, block_values, block_cols):
    height = left_rows.shape[0]
    all_tiles = block_values.reshape(NT, NPAN * KP, TILE, TILE)
    all_columns = (jnp.arange(NPAN, dtype=jnp.int32)[None, :, None] * ST + block_cols.reshape(NT, NPAN, KP)).reshape(NT, NPAN * KP)

    def advance(running, inputs):
        row_tiles, row_columns, tile_row = inputs
        portion = lax.dynamic_slice_in_dim(left_rows, tile_row * TILE, TILE, 1)
        product = jnp.einsum("rx,qxy->rqy", portion, row_tiles.astype(jnp.float32))
        return running.at[:, row_columns, :].add(product), None

    running = jnp.zeros((height, NT, TILE), jnp.float32)
    running, ignored = lax.scan(advance, running, (all_tiles, all_columns, jnp.arange(NT, dtype=jnp.int32)))
    return running.reshape(height, ORDER)


def reference(block_values, block_cols):
    window_index = (jnp.arange(N_GX, dtype=jnp.int32)[:, None] * RB + jnp.arange(WIN, dtype=jnp.int32)[None, :]).reshape(-1)
    left_rows = dense_rows(block_values[0][window_index], block_cols[0][window_index])
    square = times_matrix(left_rows, block_values, block_cols)
    rounded = lax.optimization_barrier(square.astype(jnp.bfloat16)).astype(jnp.float32)
    return 3.0 * square - 2.0 * times_matrix(rounded, block_values, block_cols)
```

```python
import functools

import jax
import jax.numpy as jnp
from jax import lax
from jax.experimental import pallas as pl
from jax.experimental.pallas import tpu as pltpu
from jax.sharding import PartitionSpec as P

MESH = pl.DeviceIdType.MESH
F32, BF16 = jnp.float32, jnp.bfloat16
NZ, NX, NY = 8, 4, 4
RB, KP, T = 4, 6, 128
Q = T // NX
ROWS = NZ * Q
HALF = ROWS // 2
UNITS = ((0, 0), (0, 1), (1, 0), (2, 1), (1, 1), (2, 0), (3, 0), (3, 1))


def where_am_i():
    g = lax.axis_index("gx")
    return g // 2, lax.rem(g, 2), lax.axis_index("gy"), lax.axis_index("gz")


def at_z(z, c):
    return {"gx": lax.rem(z + 2 * NZ, NZ) * 2 + c}


def greet(devices):
    barrier = pltpu.get_barrier_semaphore()
    for device in devices:
        pl.semaphore_signal(barrier, inc=1, device_id=device, device_id_type=MESH)
    pl.semaphore_wait(barrier, len(devices))


def nt_dot(a, b):
    return lax.dot_general(a, b, (((1,), (1,)), ((), ())), preferred_element_type=F32)


def front(v_ref, c_ref, p_out, s_out, cp_out,
          pall, lq, cw, cp, mapv, maps, cps, sp, sb, relay, parts, fwd, sfin,
          xs, xr, ds, dr, cs, cr, ls, lr, ws, wr, ys, yr, loc, outs):
    z, c, x, y = where_am_i()
    sib = 1 - c
    xright, xleft, xopp = lax.rem(x + 1, NX), lax.rem(x + 3, NX), lax.rem(x + 2, NX)
    yright, yleft, yopp = lax.rem(y + 1, NY), lax.rem(y + 3, NY), lax.rem(y + 2, NY)
    me2 = {"gx": z * 2 + sib}

    def remote(src, dst, ssem, rsem, device):
        return pltpu.make_async_remote_copy(
            src_ref=src, dst_ref=dst, send_sem=ssem, recv_sem=rsem,
            device_id=device, device_id_type=MESH)

    col_peers = []
    for dx in range(NX):
        for dc in range(2):
            if dx or dc:
                col_peers.append((dx, dc, {"gx": z * 2 + lax.rem(c + dc, 2), "gy": lax.rem(x + dx, NX)}))
    greet([p[2] for p in col_peers] + [at_z(z + d, c) for d in range(1, NZ)]
          + [{"gz": yright}, {"gz": yleft}])

    started = []

    def go(copy):
        copy.start()
        started.append(copy)
        return copy

    def left_copy(dx):
        return remote(v_ref.at[0, :, pl.ds(dx * Q, Q), :], lq.at[z, 0:KP], ls.at[dx], lr.at[0], {"gy": dx})

    def leftc_copy(dx):
        return remote(c_ref, cw.at[z], ls.at[NX + dx], lr.at[1], {"gy": dx})

    @pl.when(x == 0)
    def _():
        for dx in range(1, NX):
            left_copy(dx).start()
            leftc_copy(dx).start()

    xsend = {}
    for order in range(2):
        for way, half, dev in ((0, order, xright), (1, 1 - order, xleft)):
            rows = pl.ds(2 * half, 2)
            xsend[way, half] = go(remote(v_ref.at[rows], pall.at[1 + way, c, rows],
                                         xs.at[way, half], xr.at[way, half], {"gy": dev}))
    dsend = {}
    for half in range(2):
        rows = pl.ds(2 * half, 2)
        dsend[0, half] = go(remote(v_ref.at[rows], pall.at[0, c, rows], ds.at[0, half], dr.at[0, half], me2))
    csend = []
    for n, (dx, dc, dev) in enumerate(col_peers):
        rel = {0: 0, 1: 1, 2: 3, 3: 2}[dx]
        csend.append(go(remote(c_ref, cp.at[rel, c], cs.at[n], cr.at[n], dev)))
    cp[0, c] = c_ref[...]
    for r in range(RB):
        pall[0, c, r] = v_ref[r]
    for zz in range(NZ):
        lq[zz, KP] = jnp.zeros((Q, T), BF16)

    @pl.when(x == 0)
    def _():
        lq[z, 0:KP] = v_ref[0, :, 0:Q, :]
        cw[z] = c_ref[...]
        for dx in range(1, NX):
            left_copy(dx).wait_send()
            leftc_copy(dx).wait_send()

    @pl.when(x != 0)
    def _():
        left_copy(0).wait_recv()
        leftc_copy(0).wait_recv()

    wsend = []
    for d in range(1, NZ):
        wsend.append(go(remote(lq.at[z, 0:KP], lq.at[z, 0:KP], ws.at[0, d], wr.at[0, d], at_z(z + d, c))))
        wsend.append(go(remote(cw.at[z], cw.at[z], ws.at[1, d], wr.at[1, d], at_z(z + d, c))))
    for copy in csend:
        copy.wait_recv()
    to_smem = pltpu.make_async_copy(cp, cps, loc.at[0])
    to_smem.start()
    for copy in wsend:
        copy.wait_recv()
    lane = lax.broadcasted_iota(jnp.int32, (1, T), 1)
    for zz in range(NZ):
        row = cw[zz]
        found = jnp.full((1, T), KP, jnp.int32)
        for k in range(KP):
            found = jnp.where(jnp.broadcast_to(row[:, k : k + 1], (1, T)) == lane, k, found)
        mapv[zz] = found
    map_copy = pltpu.make_async_copy(mapv, maps, loc.at[1])
    map_copy.start()
    to_smem.wait()
    map_copy.wait()
    cols_out = pltpu.make_async_copy(cp, cp_out, outs.at[0])
    cols_out.start()

    def square_part(rel, half):
        u = rel * 2 + half

        def body(n, carry):
            block, r = n // 2, lax.rem(n, 2)
            row = 2 * half + r
            wide = []
            for k in range(KP):
                col = cps[rel, block, 0, row * KP + k]
                wide.append(jnp.concatenate([lq[zz, maps[zz, 0, col]] for zz in range(NZ)], axis=0))
            total = None
            for k in range(0, KP, 2):
                lhs = jnp.concatenate(wide[k : k + 2], axis=1)
                rhs = jnp.concatenate([pall[rel, block, row, k], pall[rel, block, row, k + 1]], axis=1)
                prod = nt_dot(lhs, rhs)
                total = prod if total is None else total + prod
            sp[u, n] = total
            sb[u, n] = total.astype(BF16)
            return carry

        lax.fori_loop(0, 4, body, 0)

    top, bottom = pl.ds(0, HALF), pl.ds(HALF, HALF)
    R, L = {"gz": yright}, {"gz": yleft}

    def ycopy(u, m, src, dst, dev):
        return remote(src, dst, ys.at[u, m], yr.at[u, m], dev)

    def message(u, m):
        if m == 0:
            return ycopy(u, 0, sb.at[u, yopp, bottom], relay.at[u, 0], R)
        if m == 1:
            return ycopy(u, 1, sb.at[u, yopp, top], relay.at[u, 1], L)
        if m == 2:
            return ycopy(u, 2, sb.at[u, yright, top], parts.at[u, 0], R)
        if m == 3:
            return ycopy(u, 3, sb.at[u, yleft, bottom], parts.at[u, 1], L)
        if m == 4:
            return ycopy(u, 4, fwd.at[u, 0], parts.at[u, 2], R)
        if m == 5:
            return ycopy(u, 5, fwd.at[u, 1], parts.at[u, 3], L)
        if m in (6, 7):
            rows = top if m == 6 else bottom
            return ycopy(u, m, sfin.at[u, y, rows], sfin.at[u, y, rows], R)
        if m in (8, 9):
            rows = top if m == 8 else bottom
            return ycopy(u, m, sfin.at[u, y, rows], sfin.at[u, y, rows], L)
        if m == 10:
            return ycopy(u, 10, sfin.at[u, yleft, top], sfin.at[u, yleft, top], R)
        return ycopy(u, 11, sfin.at[u, yright, bottom], sfin.at[u, yright, bottom], L)

    def send_parts(u):
        for m in range(4):
            go(message(u, m))

    def send_relay(u):
        message(u, 0).wait_recv()
        fwd[u, 0] = (sp[u, yright, HALF:ROWS] + relay[u, 0].astype(F32)).astype(BF16)
        go(message(u, 4))
        message(u, 1).wait_recv()
        fwd[u, 1] = (sp[u, yleft, 0:HALF] + relay[u, 1].astype(F32)).astype(BF16)
        go(message(u, 5))

    def send_sum(u):
        message(u, 2).wait_recv()
        message(u, 5).wait_recv()
        sfin[u, y, 0:HALF] = (sp[u, y, 0:HALF] + parts[u, 0].astype(F32) + parts[u, 3].astype(F32)).astype(BF16)
        go(message(u, 6))
        go(message(u, 8))
        message(u, 3).wait_recv()
        message(u, 4).wait_recv()
        sfin[u, y, HALF:ROWS] = (sp[u, y, HALF:ROWS] + parts[u, 1].astype(F32) + parts[u, 2].astype(F32)).astype(BF16)
        go(message(u, 9))
        go(message(u, 7))

    def send_forward(u):
        message(u, 6).wait_recv()
        go(message(u, 10))
        message(u, 9).wait_recv()
        go(message(u, 11))

    def finish(u):
        for m in (7, 8, 10, 11):
            message(u, m).wait_recv()
        copy = pltpu.make_async_copy(sfin.at[u], s_out.at[u], outs.at[5 + u])
        copy.start()
        return copy

    final = [cols_out]

    def arrive(rel, half):
        rows = pl.ds(2 * half, 2)
        dsend[rel, half] = go(remote(pall.at[rel, c, rows], pall.at[rel, c, rows],
                                     ds.at[rel, half], dr.at[rel, half], me2))

    def p_done(rel):
        copy = pltpu.make_async_copy(pall.at[rel], p_out.at[rel], outs.at[1 + rel])
        copy.start()
        final.append(copy)

    def u_of(rel, half):
        return rel * 2 + half

    for half in range(2):
        dsend[0, half].wait_recv()
        square_part(0, half)
        send_parts(u_of(0, half))
    p_done(0)
    xsend[0, 0].wait_recv()
    rows = pl.ds(0, 2)
    xsend[2, 0] = go(remote(pall.at[1, c, rows], pall.at[3, c, rows], xs.at[2, 0], xr.at[2, 0], {"gy": xright}))
    arrive(1, 0)
    xsend[1, 1].wait_recv()
    rows = pl.ds(2, 2)
    xsend[2, 1] = go(remote(pall.at[2, c, rows], pall.at[3, c, rows], xs.at[2, 1], xr.at[2, 1], {"gy": xleft}))
    arrive(2, 1)
    for half in range(2):
        send_relay(u_of(0, half))
    for rel, half in ((1, 0), (2, 1)):
        dsend[rel, half].wait_recv()
        square_part(rel, half)
        send_parts(u_of(rel, half))
    for half in range(2):
        send_sum(u_of(0, half))
    for rel, half in ((1, 0), (2, 1)):
        send_relay(u_of(rel, half))
    xsend[0, 1].wait_recv()
    arrive(1, 1)
    xsend[1, 0].wait_recv()
    arrive(2, 0)
    for half in range(2):
        send_forward(u_of(0, half))
    for rel, half in ((1, 1), (2, 0)):
        dsend[rel, half].wait_recv()
        square_part(rel, half)
        send_parts(u_of(rel, half))
    p_done(1)
    p_done(2)
    for rel, half in ((1, 0), (2, 1)):
        send_sum(u_of(rel, half))
    for rel, half in ((1, 1), (2, 0)):
        send_relay(u_of(rel, half))
    xsend[2, 0].wait_recv()
    arrive(3, 0)
    xsend[2, 1].wait_recv()
    arrive(3, 1)
    for rel, half in ((3, 0), (3, 1)):
        dsend[rel, half].wait_recv()
        square_part(rel, half)
        send_parts(u_of(rel, half))
    p_done(3)
    for rel, half in ((1, 0), (2, 1)):
        send_forward(u_of(rel, half))
    for rel, half in ((1, 1), (2, 0)):
        send_sum(u_of(rel, half))
    for half in range(2):
        send_relay(u_of(3, half))
    for half in range(2):
        final.append(finish(u_of(0, half)))
    for rel, half in ((1, 1), (2, 0)):
        send_forward(u_of(rel, half))
    for half in range(2):
        send_sum(u_of(3, half))
    for rel, half in ((1, 0), (2, 1)):
        final.append(finish(u_of(rel, half)))
    for half in range(2):
        send_forward(u_of(3, half))
    for rel, half in ((1, 1), (2, 0), (3, 0), (3, 1)):
        final.append(finish(u_of(rel, half)))
    for copy in started:
        copy.wait_send()
    for copy in final:
        copy.wait()


def middle(cols, p_ref, s_ref, r_ref, acc):
    n = pl.program_id(0)
    rel, block = n // 2, lax.rem(n, 2)
    z, c, x, y = where_am_i()

    @pl.when(n == 0)
    def _():
        acc[...] = jnp.zeros_like(acc)

    slab = lax.rem(x + jnp.where(rel == 0, 0, jnp.where(rel == 1, NX - 1, jnp.where(rel == 2, 1, 2))), NX)

    @pl.when(slab == y)
    def _():
        for r in range(RB):
            mine = s_ref[r // 2, block * 2 + r % 2].astype(F32)
            at = 8 * z + 4 * block + r
            acc[at] += -1.5 * mine

    def body(r, carry):
        mine = s_ref[r // 2, block * 2 + lax.rem(r, 2)]
        for k in range(KP):
            col = cols[rel, block, 0, r * KP + k]
            acc[col] += jnp.dot(mine, p_ref[0, 0, r, k], preferred_element_type=F32)
        return carry

    lax.fori_loop(0, RB, body, 0)

    @pl.when(n == 2 * NX - 1)
    def _():
        def out(j, carry):
            tile = (-2.0 * acc[j]).astype(BF16)
            for zz in range(NZ):
                r_ref[zz, j] = tile[zz * Q : (zz + 1) * Q]
            return carry

        lax.fori_loop(0, 64, out, 0)


SUBS = 8
PER = 64 // SUBS


def back(r_ref, o_ref, rbuf, sbuf, ssem, rsem):
    z, c, x, y = where_am_i()
    devs = (at_z(z + 1, c), at_z(z - 1, c))
    greet(devs)

    def tiles(sub):
        return pl.ds(sub * PER, PER)

    def copy(way, step, sub, src):
        return pltpu.make_async_remote_copy(
            src_ref=src, dst_ref=rbuf.at[way, step, sub],
            send_sem=ssem.at[way, step, sub], recv_sem=rsem.at[way, step, sub],
            device_id=devs[way], device_id_type=MESH)

    started = []
    relays = (range(0, SUBS // 2), range(SUBS // 2, SUBS))
    for step in range(4):
        dest = (lax.rem(z + 4 - step, NZ), lax.rem(z + 4 + step, NZ))
        for pos in range(SUBS):
            for way in range(2):
                sub = pos if way == 0 else (pos + SUBS // 2) % SUBS
                first = sub in relays[way]
                if step == 0 and not first:
                    continue
                own = r_ref.at[dest[way], tiles(sub)]
                if step == 0 or (step == 1 and not first):
                    move = copy(way, step, sub, own)
                else:
                    copy(way, step - 1, sub, own).wait_recv()
                    sbuf[way, step, sub] = (own[...].astype(F32) + rbuf[way, step - 1, sub].astype(F32)).astype(BF16)
                    move = copy(way, step, sub, sbuf.at[way, step, sub])
                move.start()
                started.append(move)
    for sub in range(SUBS):
        for way in range(2):
            copy(way, 3, sub, sbuf.at[way, 3, sub]).wait_recv()
        total = (r_ref[z, tiles(sub)].astype(F32) + rbuf[0, 3, sub].astype(F32) + rbuf[1, 3, sub].astype(F32))
        for t in range(PER):
            j = sub * PER + t
            o_ref[:, j * T : (j + 1) * T] = total[t]
    for move in started:
        move.wait_send()


def local(block_values, block_cols):
    v = block_values[0, :, 0]
    cflat = jnp.pad(block_cols.reshape(1, RB * KP), ((0, 0), (0, T - RB * KP)))
    vmem = pl.BlockSpec(memory_space=pltpu.VMEM)
    anys = pl.BlockSpec(memory_space=pl.ANY)
    sem = pltpu.SemaphoreType.DMA
    p_all, s_all, cols = pl.pallas_call(
        front,
        out_shape=(
            jax.ShapeDtypeStruct((NX, 2, RB, KP, T, T), BF16),
            jax.ShapeDtypeStruct((8, 4, ROWS, T), BF16),
            jax.ShapeDtypeStruct((NX, 2, 1, T), jnp.int32),
        ),
        in_specs=[vmem, vmem],
        out_specs=(anys, anys, anys),
        scratch_shapes=[
            pltpu.VMEM((NX, 2, RB, KP, T, T), BF16),
            pltpu.VMEM((NZ, KP + 1, Q, T), BF16),
            pltpu.VMEM((NZ, 1, T), jnp.int32),
            pltpu.VMEM((NX, 2, 1, T), jnp.int32),
            pltpu.VMEM((NZ, 1, T), jnp.int32),
            pltpu.SMEM((NZ, 1, T), jnp.int32),
            pltpu.SMEM((NX, 2, 1, T), jnp.int32),
            pltpu.VMEM((8, 4, ROWS, T), F32),
            pltpu.VMEM((8, 4, ROWS, T), BF16),
            pltpu.VMEM((8, 2, HALF, T), BF16),
            pltpu.VMEM((8, 4, HALF, T), BF16),
            pltpu.VMEM((8, 2, HALF, T), BF16),
            pltpu.VMEM((8, 4, ROWS, T), BF16),
            sem((3, 2)), sem((3, 2)), sem((4, 2)), sem((4, 2)),
            sem((7,)), sem((7,)), sem((8,)), sem((2,)),
            sem((2, NZ)), sem((2, NZ)), sem((8, 12)), sem((8, 12)),
            sem((2,)), sem((13,)),
        ],
        compiler_params=pltpu.CompilerParams(
            collective_id=0, has_side_effects=True, vmem_limit_bytes=40 << 20),
        name="front",
    )(v, cflat)
    r_all = pl.pallas_call(
        middle,
        out_shape=jax.ShapeDtypeStruct((NZ, 64, Q, T), BF16),
        grid=(8,),
        in_specs=[
            pl.BlockSpec(memory_space=pltpu.SMEM),
            pl.BlockSpec((1, 1, RB, KP, T, T), lambda n: (n // 2, n % 2, 0, 0, 0, 0)),
            pl.BlockSpec((2, 4, ROWS, T), lambda n: (n // 2, 0, 0, 0)),
        ],
        out_specs=vmem,
        scratch_shapes=[pltpu.VMEM((64, ROWS, T), F32)],
        compiler_params=pltpu.CompilerParams(
            dimension_semantics=("arbitrary",), vmem_limit_bytes=40 << 20),
        name="middle",
    )(cols, p_all, s_all)
    return pl.pallas_call(
        back,
        out_shape=jax.ShapeDtypeStruct((Q, 64 * T), F32),
        in_specs=[vmem],
        out_specs=vmem,
        scratch_shapes=[
            pltpu.VMEM((2, 4, SUBS, PER, Q, T), BF16),
            pltpu.VMEM((2, 4, SUBS, PER, Q, T), BF16),
            sem((2, 4, SUBS)), sem((2, 4, SUBS)),
        ],
        compiler_params=pltpu.CompilerParams(
            collective_id=1, has_side_effects=True, vmem_limit_bytes=40 << 20),
        name="back",
    )(r_all)


def solution(mesh):
    in_specs = (P("gy", "gx", "gz", None, None, None), P("gy", "gx", "gz", None))
    return jax.shard_map(local, mesh=mesh, in_specs=in_specs, out_specs=P(("gx", "gy"), "gz"), check_vma=False)
```

```python
import functools

import jax
import jax.numpy as jnp
from jax import lax
from jax.experimental import pallas as pl
from jax.experimental.pallas import tpu as pltpu
from jax.sharding import PartitionSpec as P

MESH = pl.DeviceIdType.MESH
F32, BF16 = jnp.float32, jnp.bfloat16
NZ, NX, NY = 8, 4, 4
RB, KP, T = 4, 6, 128
Q = T // NX
ROWS = NZ * Q
HALF = ROWS // 2
TILES = NX * 2 * RB * KP
SUBS = 8
PER = 64 // SUBS
UNITS = ((0, 0), (0, 1), (1, 0), (2, 1), (1, 1), (2, 0), (3, 0), (3, 1))


def where_am_i():
    g = lax.axis_index("gx")
    return g // 2, lax.rem(g, 2), lax.axis_index("gy"), lax.axis_index("gz")


def at_z(z, c):
    return {"gx": lax.rem(z + 2 * NZ, NZ) * 2 + c}


def greet(devices):
    barrier = pltpu.get_barrier_semaphore()
    for device in devices:
        pl.semaphore_signal(barrier, inc=1, device_id=device, device_id_type=MESH)
    pl.semaphore_wait(barrier, len(devices))


def nt_dot(a, b):
    return lax.dot_general(a, b, (((1,), (1,)), ((), ())), preferred_element_type=F32)


def sort_tiles(cp, colv, prev, ordv):
    for n in range(2 * NX * RB):
        colv[n : n + 1, :] = cp[n // 8, n // 4 % 2, n % 4]
    count = 2 * NX * RB
    cols = colv[...]
    lanes = lax.broadcasted_iota(jnp.int32, (count, T), 1)
    hits = [jnp.broadcast_to(cols[:, k : k + 1], (count, T)) == lanes for k in range(KP)]
    listed = jnp.zeros((count, T), jnp.int32)
    for hit in hits:
        listed = listed + jnp.where(hit, 1, 0)
    run = jnp.zeros((1, T), jnp.int32)
    for n in range(count):
        prev[n : n + 1, :] = run
        run = run + listed[n : n + 1, :]
    lane = lax.broadcasted_iota(jnp.int32, (1, T), 1)
    upto = run
    for shift in (1, 2, 4, 8, 16, 32, 64):
        upto = upto + jnp.where(lane >= shift, pltpu.roll(upto, shift, 1), 0)
    before = prev[...]
    place = (jnp.broadcast_to(upto - run, (count, T)) + before) * 2 + jnp.where(before > 0, 1, 0)
    ordv[2] = jnp.where(run > 0, upto - 1, TILES)
    tile = lax.broadcasted_iota(jnp.int32, (count, T), 0) * KP
    picked = [jnp.zeros((count, T), jnp.int32) for part in range(2)]
    for k, hit in enumerate(hits):
        mine = jnp.sum(jnp.where(hit, place, 0), axis=1, keepdims=True)
        mine = jnp.broadcast_to(mine, (count, T))
        code = (tile + k) * 2 + jnp.where(lax.rem(mine, 2) == 1, 1, 0)
        for part in range(2):
            picked[part] = jnp.where(mine // 2 == lanes + part * T, code, picked[part])
    for part in range(2):
        ordv[part] = jnp.sum(picked[part], axis=0, keepdims=True)


def step(v_hbm, c_in, o_ref,
         v_ref, c_ref, pall, lq, cw, cp, mapv, maps, cps, sp, sb, relay, parts, fwd, sfin,
         colv, prev, ordv, ords, prods, sums, rbuf, sbuf,
         xs, xr, ds, dr, cs, cr, ls, lr, ws, wr, ys, yr, loc, zs, zr):
    z, c, x, y = where_am_i()
    sib = 1 - c
    xright, xleft, xopp = lax.rem(x + 1, NX), lax.rem(x + 3, NX), lax.rem(x + 2, NX)
    yright, yleft, yopp = lax.rem(y + 1, NY), lax.rem(y + 3, NY), lax.rem(y + 2, NY)
    me2 = {"gx": z * 2 + sib}

    def remote(src, dst, ssem, rsem, device):
        return pltpu.make_async_remote_copy(
            src_ref=src, dst_ref=dst, send_sem=ssem, recv_sem=rsem,
            device_id=device, device_id_type=MESH)

    fetch = pltpu.make_async_copy(v_hbm, v_ref, loc.at[2])
    fetch.start()
    for r in range(RB):
        c_ref[r] = jnp.zeros((1, T), jnp.int32)
        c_ref[r, :, 0:KP] = c_in[0, r]

    col_peers = []
    for dx in range(NX):
        for dc in range(2):
            if dx or dc:
                col_peers.append((dx, dc, {"gx": z * 2 + lax.rem(c + dc, 2), "gy": lax.rem(x + dx, NX)}))
    greet([p[2] for p in col_peers] + [at_z(z + d, c) for d in range(1, NZ)]
          + [{"gz": yright}, {"gz": yleft}])

    fetch.wait()
    started = []

    def go(copy):
        copy.start()
        started.append(copy)
        return copy

    def left_copy(dx):
        return remote(v_ref.at[0, :, pl.ds(dx * Q, Q), :], lq.at[z, 0:KP], ls.at[dx], lr.at[0], {"gy": dx})

    def leftc_copy(dx):
        return remote(c_ref.at[0], cw.at[z], ls.at[NX + dx], lr.at[1], {"gy": dx})

    @pl.when(x == 0)
    def _():
        for dx in range(1, NX):
            left_copy(dx).start()
            leftc_copy(dx).start()

    xsend = {}
    for order in range(2):
        for way, half, dev in ((0, order, xright), (1, 1 - order, xleft)):
            rows = pl.ds(2 * half, 2)
            xsend[way, half] = go(remote(v_ref.at[rows], pall.at[1 + way, c, rows],
                                         xs.at[way, half], xr.at[way, half], {"gy": dev}))
    dsend = {}
    for half in range(2):
        rows = pl.ds(2 * half, 2)
        dsend[0, half] = go(remote(v_ref.at[rows], pall.at[0, c, rows], ds.at[0, half], dr.at[0, half], me2))
    csend = []
    for n, (dx, dc, dev) in enumerate(col_peers):
        rel = {0: 0, 1: 1, 2: 3, 3: 2}[dx]
        csend.append(go(remote(c_ref, cp.at[rel, c], cs.at[n], cr.at[n], dev)))
    cp[0, c] = c_ref[...]
    for r in range(RB):
        pall[0, c, r] = v_ref[r]
    for zz in range(NZ):
        lq[zz, KP] = jnp.zeros((Q, T), BF16)

    @pl.when(x == 0)
    def _():
        lq[z, 0:KP] = v_ref[0, :, 0:Q, :]
        cw[z] = c_ref[0]
        for dx in range(1, NX):
            left_copy(dx).wait_send()
            leftc_copy(dx).wait_send()

    @pl.when(x != 0)
    def _():
        left_copy(0).wait_recv()
        leftc_copy(0).wait_recv()

    wsend = []
    for d in range(1, NZ):
        wsend.append(go(remote(lq.at[z, 0:KP], lq.at[z, 0:KP], ws.at[0, d], wr.at[0, d], at_z(z + d, c))))
        wsend.append(go(remote(cw.at[z], cw.at[z], ws.at[1, d], wr.at[1, d], at_z(z + d, c))))
    for copy in csend:
        copy.wait_recv()
    to_smem = pltpu.make_async_copy(cp, cps, loc.at[0])
    to_smem.start()
    for copy in wsend:
        copy.wait_recv()
    lane = lax.broadcasted_iota(jnp.int32, (1, T), 1)
    for zz in range(NZ):
        row = cw[zz]
        found = jnp.full((1, T), KP, jnp.int32)
        for k in range(KP):
            found = jnp.where(jnp.broadcast_to(row[:, k : k + 1], (1, T)) == lane, k, found)
        mapv[zz] = found
    map_copy = pltpu.make_async_copy(mapv, maps, loc.at[1])
    map_copy.start()
    to_smem.wait()
    map_copy.wait()

    def square_part(rel, half):
        u = rel * 2 + half

        def body(n, carry):
            block, r = n // 2, lax.rem(n, 2)
            row = 2 * half + r
            wide = []
            for k in range(KP):
                col = cps[rel, block, row, 0, k]
                wide.append(jnp.concatenate([lq[zz, maps[zz, 0, col]] for zz in range(NZ)], axis=0))
            total = None
            for k in range(0, KP, 2):
                lhs = jnp.concatenate(wide[k : k + 2], axis=1)
                rhs = jnp.concatenate([pall[rel, block, row, k], pall[rel, block, row, k + 1]], axis=1)
                prod = nt_dot(lhs, rhs)
                total = prod if total is None else total + prod
            sp[u, n] = total
            sb[u, n] = total.astype(BF16)
            return carry

        lax.fori_loop(0, 4, body, 0)

    top, bottom = pl.ds(0, HALF), pl.ds(HALF, HALF)
    R, L = {"gz": yright}, {"gz": yleft}

    def ycopy(u, m, src, dst, dev):
        return remote(src, dst, ys.at[u, m], yr.at[u, m], dev)

    def message(u, m):
        if m == 0:
            return ycopy(u, 0, sb.at[u, yopp, bottom], relay.at[u, 0], R)
        if m == 1:
            return ycopy(u, 1, sb.at[u, yopp, top], relay.at[u, 1], L)
        if m == 2:
            return ycopy(u, 2, sb.at[u, yright, top], parts.at[u, 0], R)
        if m == 3:
            return ycopy(u, 3, sb.at[u, yleft, bottom], parts.at[u, 1], L)
        if m == 4:
            return ycopy(u, 4, fwd.at[u, 0], parts.at[u, 2], R)
        if m == 5:
            return ycopy(u, 5, fwd.at[u, 1], parts.at[u, 3], L)
        if m in (6, 7):
            rows = top if m == 6 else bottom
            return ycopy(u, m, sfin.at[u, y, rows], sfin.at[u, y, rows], R)
        if m in (8, 9):
            rows = top if m == 8 else bottom
            return ycopy(u, m, sfin.at[u, y, rows], sfin.at[u, y, rows], L)
        if m == 10:
            return ycopy(u, 10, sfin.at[u, yleft, top], sfin.at[u, yleft, top], R)
        return ycopy(u, 11, sfin.at[u, yright, bottom], sfin.at[u, yright, bottom], L)

    def send_parts(u):
        for m in range(4):
            go(message(u, m))

    def send_relay(u):
        message(u, 0).wait_recv()
        fwd[u, 0] = (sp[u, yright, HALF:ROWS] + relay[u, 0].astype(F32)).astype(BF16)
        go(message(u, 4))
        message(u, 1).wait_recv()
        fwd[u, 1] = (sp[u, yleft, 0:HALF] + relay[u, 1].astype(F32)).astype(BF16)
        go(message(u, 5))

    def send_sum(u):
        message(u, 2).wait_recv()
        message(u, 5).wait_recv()
        sfin[u, y, 0:HALF] = (sp[u, y, 0:HALF] + parts[u, 0].astype(F32) + parts[u, 3].astype(F32)).astype(BF16)
        go(message(u, 6))
        go(message(u, 8))
        message(u, 3).wait_recv()
        message(u, 4).wait_recv()
        sfin[u, y, HALF:ROWS] = (sp[u, y, HALF:ROWS] + parts[u, 1].astype(F32) + parts[u, 2].astype(F32)).astype(BF16)
        go(message(u, 9))
        go(message(u, 7))

    def send_forward(u):
        message(u, 6).wait_recv()
        go(message(u, 10))
        message(u, 9).wait_recv()
        go(message(u, 11))

    def finish(u):
        for m in (7, 8, 10, 11):
            message(u, m).wait_recv()


    def arrive(rel, half):
        rows = pl.ds(2 * half, 2)
        dsend[rel, half] = go(remote(pall.at[rel, c, rows], pall.at[rel, c, rows],
                                     ds.at[rel, half], dr.at[rel, half], me2))

    def products(rel, half):
        u = rel * 2 + half

        def body(n, carry):
            block, r = n // 2, lax.rem(n, 2)
            row = 2 * half + r
            wide = jnp.concatenate([pall[rel, block, row, k] for k in range(KP)], axis=1)
            both = jnp.dot(sfin[u, n], wide, preferred_element_type=F32)
            at = ((rel * 2 + block) * RB + row) * KP
            for k in range(KP):
                prods[at + k] = both[:, k * T : (k + 1) * T]
            return carry

        lax.fori_loop(0, 4, body, 0)

    def u_of(rel, half):
        return rel * 2 + half

    for half in range(2):
        dsend[0, half].wait_recv()
        square_part(0, half)
        send_parts(u_of(0, half))
    sort_tiles(cp, colv, prev, ordv)
    order_copy = pltpu.make_async_copy(ordv, ords, loc.at[0])
    order_copy.start()
    xsend[0, 0].wait_recv()
    rows = pl.ds(0, 2)
    xsend[2, 0] = go(remote(pall.at[1, c, rows], pall.at[3, c, rows], xs.at[2, 0], xr.at[2, 0], {"gy": xright}))
    arrive(1, 0)
    xsend[1, 1].wait_recv()
    rows = pl.ds(2, 2)
    xsend[2, 1] = go(remote(pall.at[2, c, rows], pall.at[3, c, rows], xs.at[2, 1], xr.at[2, 1], {"gy": xleft}))
    arrive(2, 1)
    for half in range(2):
        send_relay(u_of(0, half))
    for rel, half in ((1, 0), (2, 1)):
        dsend[rel, half].wait_recv()
        square_part(rel, half)
        send_parts(u_of(rel, half))
    for half in range(2):
        send_sum(u_of(0, half))
    for rel, half in ((1, 0), (2, 1)):
        send_relay(u_of(rel, half))
    xsend[0, 1].wait_recv()
    arrive(1, 1)
    xsend[1, 0].wait_recv()
    arrive(2, 0)
    for half in range(2):
        send_forward(u_of(0, half))
    for rel, half in ((1, 1), (2, 0)):
        dsend[rel, half].wait_recv()
        square_part(rel, half)
        send_parts(u_of(rel, half))
    for rel, half in ((1, 0), (2, 1)):
        send_sum(u_of(rel, half))
    for rel, half in ((1, 1), (2, 0)):
        send_relay(u_of(rel, half))
    for rel, half in ((1, 0), (2, 1)):
        send_forward(u_of(rel, half))
    for rel, half in ((1, 1), (2, 0)):
        send_sum(u_of(rel, half))
    xsend[2, 0].wait_recv()
    arrive(3, 0)
    xsend[2, 1].wait_recv()
    arrive(3, 1)
    for half in range(2):
        finish(u_of(0, half))
        products(0, half)
    for rel, half in ((3, 0), (3, 1)):
        dsend[rel, half].wait_recv()
        square_part(rel, half)
        send_parts(u_of(rel, half))
    for rel, half in ((1, 1), (2, 0)):
        send_forward(u_of(rel, half))
    for rel, half in ((1, 0), (2, 1)):
        finish(u_of(rel, half))
        products(rel, half)
    for half in range(2):
        send_relay(u_of(3, half))
    for half in range(2):
        send_sum(u_of(3, half))
    for half in range(2):
        send_forward(u_of(3, half))
    for rel, half in ((1, 1), (2, 0), (3, 0), (3, 1)):
        finish(u_of(rel, half))
        products(rel, half)
    order_copy.wait()
    zdevs = (at_z(z + 1, c), at_z(z - 1, c))
    ahead = lax.rem(y - x + NX, NX)
    here = jnp.where(ahead == 0, 0, jnp.where(ahead == 3, 1, jnp.where(ahead == 1, 2, 3)))

    def rows_of(dest):
        return pl.ds(pl.multiple_of(dest * Q, Q), Q)

    def scan(way, dest):
        rows = rows_of(dest)
        run = jnp.zeros((Q, T), F32)
        for part in range(2):
            def body(n, run, part=part):
                for m in range(8):
                    t = n * 8 + m
                    code = ords[part, 0, t]
                    tile = prods[code // 2, rows]
                    run = tile + run * lax.rem(code, 2).astype(F32)
                    sums[way, part * T + t] = run
                return run

            run = lax.fori_loop(0, 16 if part == 0 else TILES // 8 - 16, body, run)
        for n in range(2 * RB):
            last = ords[2, 0, 8 * z + n]
            mine = sfin[here * 2 + n % 4 // 2, n // 4 * 2 + n % 2, rows].astype(F32)
            sums[way, TILES + 1 + n] = sums[way, last] - 1.5 * mine

    def result_tile(way, j):
        own = j - 8 * z
        inside = jnp.logical_and(own >= 0, own < 8)
        return -2.0 * sums[way, jnp.where(inside, TILES + 1 + own, ords[2, 0, j])]

    def zcopy(way, hop, sub):
        return pltpu.make_async_remote_copy(
            src_ref=sbuf.at[way, hop, sub], dst_ref=rbuf.at[way, hop, sub],
            send_sem=zs.at[way, hop, sub], recv_sem=zr.at[way, hop, sub],
            device_id=zdevs[way], device_id_type=MESH)

    def emit(way, hop, sub, have):
        if have:
            zcopy(way, hop - 1, sub).wait_recv()
        for t in range(PER):
            tile = result_tile(0 if hop == 0 else way, sub * PER + t)
            if have:
                tile = tile + rbuf[way, hop - 1, sub, t].astype(F32)
            sbuf[way, hop, sub, t] = tile.astype(BF16)
        zcopy(way, hop, sub).start()

    for way in range(2):
        sums[way, TILES] = jnp.zeros((Q, T), F32)
    hs = SUBS // 2
    scan(0, lax.rem(z + 4, NZ))

    def hop0(n, carry):
        emit(0, 0, n, False)
        emit(1, 0, n + hs, False)
        return carry

    lax.fori_loop(0, hs, hop0, 0)
    for hop in range(1, 4):
        scan(0, lax.rem(z + 4 - hop, NZ))
        scan(1, lax.rem(z + 4 + hop, NZ))

        def fresh(n, carry, hop=hop):
            emit(0, hop, n + hs, hop > 1)
            emit(1, hop, n, hop > 1)
            return carry

        def relayed(n, carry, hop=hop):
            emit(0, hop, n, True)
            emit(1, hop, n + hs, True)
            return carry

        lax.fori_loop(0, hs, fresh, 0)
        lax.fori_loop(0, hs, relayed, 0)
    scan(0, z)
    for n in range(SUBS):
        for way in range(2):
            sub = (n + (hs if way == 0 else 0)) % SUBS
            zcopy(way, 3, sub).wait_recv()
    for sub in range(SUBS):
        for t in range(PER):
            j = sub * PER + t
            tile = result_tile(0, j) + rbuf[0, 3, sub, t].astype(F32) + rbuf[1, 3, sub, t].astype(F32)
            o_ref[:, j * T : (j + 1) * T] = tile

    def drain(n, carry):
        for way in range(2):
            for hop in range(1, 4):
                zcopy(way, hop, n).wait_send()
        return carry

    lax.fori_loop(0, SUBS, drain, 0)

    def drain0(n, carry):
        zcopy(0, 0, n).wait_send()
        zcopy(1, 0, n + hs).wait_send()
        return carry

    lax.fori_loop(0, hs, drain0, 0)
    for copy in started:
        copy.wait_send()


def middle(cols, p_ref, s_ref, r_ref, acc):
    n = pl.program_id(0)
    rel, block = n // 2, lax.rem(n, 2)
    z, c, x, y = where_am_i()

    @pl.when(n == 0)
    def _():
        acc[...] = jnp.zeros_like(acc)

    slab = lax.rem(x + jnp.where(rel == 0, 0, jnp.where(rel == 1, NX - 1, jnp.where(rel == 2, 1, 2))), NX)

    @pl.when(slab == y)
    def _():
        for r in range(RB):
            mine = s_ref[r // 2, block * 2 + r % 2].astype(F32)
            at = 8 * z + 4 * block + r
            acc[at] += -1.5 * mine

    def body(r, carry):
        mine = s_ref[r // 2, block * 2 + lax.rem(r, 2)]
        for k in range(KP):
            col = cols[rel, block, r, 0, k]
            acc[col] += jnp.dot(mine, p_ref[0, 0, r, k], preferred_element_type=F32)
        return carry

    lax.fori_loop(0, RB, body, 0)

    @pl.when(n == 2 * NX - 1)
    def _():
        def out(j, carry):
            tile = (-2.0 * acc[j]).astype(BF16)
            for zz in range(NZ):
                r_ref[zz, j] = tile[zz * Q : (zz + 1) * Q]
            return carry

        lax.fori_loop(0, 64, out, 0)


def local(block_values, block_cols):
    vmem, sem = pltpu.VMEM, pltpu.SemaphoreType.DMA
    return pl.pallas_call(
        step,
        out_shape=jax.ShapeDtypeStruct((Q, 64 * T), F32),
        in_specs=[pl.BlockSpec(memory_space=pl.ANY), pl.BlockSpec(memory_space=pltpu.VMEM)],
        out_specs=pl.BlockSpec(memory_space=pltpu.VMEM),
        scratch_shapes=[
            vmem((RB, KP, T, T), BF16),
            vmem((RB, 1, T), jnp.int32),
            vmem((NX, 2, RB, KP, T, T), BF16),
            vmem((NZ, KP + 1, Q, T), BF16),
            vmem((NZ, 1, T), jnp.int32),
            vmem((NX, 2, RB, 1, T), jnp.int32),
            vmem((NZ, 1, T), jnp.int32),
            pltpu.SMEM((NZ, 1, T), jnp.int32),
            pltpu.SMEM((NX, 2, RB, 1, T), jnp.int32),
            vmem((8, 4, ROWS, T), F32),
            vmem((8, 4, ROWS, T), BF16),
            vmem((8, 2, HALF, T), BF16),
            vmem((8, 4, HALF, T), BF16),
            vmem((8, 2, HALF, T), BF16),
            vmem((8, 4, ROWS, T), BF16),
            vmem((2 * NX * RB, T), jnp.int32),
            vmem((2 * NX * RB, T), jnp.int32),
            vmem((3, 1, T), jnp.int32),
            pltpu.SMEM((3, 1, T), jnp.int32),
            vmem((TILES, ROWS, T), F32),
            vmem((2, TILES + 9, Q, T), F32),
            vmem((2, 4, SUBS, PER, Q, T), BF16),
            vmem((2, 4, SUBS, PER, Q, T), BF16),
            sem((3, 2)), sem((3, 2)), sem((4, 2)), sem((4, 2)),
            sem((7,)), sem((7,)), sem((8,)), sem((2,)),
            sem((2, NZ)), sem((2, NZ)), sem((8, 12)), sem((8, 12)),
            sem((3,)), sem((2, 4, SUBS)), sem((2, 4, SUBS)),
        ],
        compiler_params=pltpu.CompilerParams(
            collective_id=0, has_side_effects=True, vmem_limit_bytes=61 << 20),
        name="step",
    )(block_values.reshape(RB, KP, T, T), block_cols)


def solution(mesh):
    in_specs = (P("gy", "gx", "gz", None, None, None), P("gy", "gx", "gz", None))
    return jax.shard_map(local, mesh=mesh, in_specs=in_specs, out_specs=P(("gx", "gy"), "gz"), check_vma=False)
```

```python
import functools

import jax
import jax.numpy as jnp
from jax import lax
from jax.experimental import pallas as pl
from jax.experimental.pallas import tpu as pltpu
from jax.sharding import PartitionSpec as P

MESH = pl.DeviceIdType.MESH
F32, BF16 = jnp.float32, jnp.bfloat16
NZ, NX, NY = 8, 4, 4
RB, KP, T = 4, 6, 128
Q = T // NX
ROWS = NZ * Q
HALF = ROWS // 2
OFFSETS = (4, 3, -3, 2, -2, 1, -1, 0)
OWN = 7
THREE = 3 * Q
VMEM_MIB = 51
TILES = NX * 2 * RB * KP
SUBS = 8
PER = 64 // SUBS


def where_am_i():
    g = lax.axis_index("gx")
    return g // 2, lax.rem(g, 2), lax.axis_index("gy"), lax.axis_index("gz")


def at_z(z, c):
    return {"gx": lax.rem(z + 2 * NZ, NZ) * 2 + c}


def greet(devices):
    barrier = pltpu.get_barrier_semaphore()
    for device in devices:
        pl.semaphore_signal(barrier, inc=1, device_id=device, device_id_type=MESH)
    pl.semaphore_wait(barrier, len(devices))


def nt_dot(a, b):
    return lax.dot_general(a, b, (((1,), (1,)), ((), ())), preferred_element_type=F32)


def sort_tiles(cp, colv, prev, ordv):
    for n in range(2 * NX * RB):
        colv[n : n + 1, :] = cp[n // 8, n // 4 % 2, n % 4]
    count = 2 * NX * RB
    cols = colv[...]
    lanes = lax.broadcasted_iota(jnp.int32, (count, T), 1)
    hits = [jnp.broadcast_to(cols[:, k : k + 1], (count, T)) == lanes for k in range(KP)]
    listed = jnp.zeros((count, T), jnp.int32)
    for hit in hits:
        listed = listed + jnp.where(hit, 1, 0)
    run = jnp.zeros((1, T), jnp.int32)
    for n in range(count):
        prev[n : n + 1, :] = run
        run = run + listed[n : n + 1, :]
    lane = lax.broadcasted_iota(jnp.int32, (1, T), 1)
    upto = run
    for shift in (1, 2, 4, 8, 16, 32, 64):
        upto = upto + jnp.where(lane >= shift, pltpu.roll(upto, shift, 1), 0)
    before = prev[...]
    place = (jnp.broadcast_to(upto - run, (count, T)) + before) * 2 + jnp.where(before > 0, 1, 0)
    ordv[2] = jnp.where(run > 0, upto - 1, TILES)
    tile = lax.broadcasted_iota(jnp.int32, (count, T), 0) * KP
    picked = [jnp.zeros((count, T), jnp.int32) for part in range(2)]
    for k, hit in enumerate(hits):
        mine = jnp.sum(jnp.where(hit, place, 0), axis=1, keepdims=True)
        mine = jnp.broadcast_to(mine, (count, T))
        code = (tile + k) * 2 + jnp.where(lax.rem(mine, 2) == 1, 1, 0)
        for part in range(2):
            picked[part] = jnp.where(mine // 2 == lanes + part * T, code, picked[part])
    for part in range(2):
        ordv[part] = jnp.sum(picked[part], axis=0, keepdims=True)


def step(v_hbm, c_in, o_ref,
         c_ref, pall, lfar, lnear, cw, cp, mapv, maps, cps, sb, relay, parts, dparts, fwd, sfin,
         colv, prev, ordv, ords, prods, sums, rbuf, sbuf,
         xs, xr, ds, dr, cs, cr, ls, lr, ws, wr, ys, yr, loc, zs, zr):
    z, c, x, y = where_am_i()
    xright, xleft = lax.rem(x + 1, NX), lax.rem(x + 3, NX)
    yright, yleft, yopp = lax.rem(y + 1, NY), lax.rem(y + 3, NY), lax.rem(y + 2, NY)
    sib = {"gx": z * 2 + 1 - c}

    def remote(src, dst, ssem, rsem, device):
        return pltpu.make_async_remote_copy(
            src_ref=src, dst_ref=dst, send_sem=ssem, recv_sem=rsem,
            device_id=device, device_id_type=MESH)

    v_ref = pall.at[0, c]
    fetch = pltpu.make_async_copy(v_hbm, v_ref, loc.at[2])
    fetch.start()
    for r in range(RB):
        c_ref[r] = jnp.zeros((1, T), jnp.int32)
        c_ref[r, :, 0:KP] = c_in[0, r]

    col_peers = []
    for dx in range(NX):
        for dc in range(2):
            if dx or dc:
                col_peers.append((dx, dc, {"gx": z * 2 + lax.rem(c + dc, 2), "gy": lax.rem(x + dx, NX)}))
    greet([p[2] for p in col_peers] + [at_z(z + d, c) for d in range(1, NZ)]
          + [{"gz": yright}, {"gz": yleft}, {"gz": yopp}])
    fetch.wait()
    started = []

    def slot(p):
        return lfar.at[p] if p < 5 else lnear.at[p - 5]

    def go(copy):
        copy.start()
        started.append(copy)
        return copy

    csend = []
    for n, (dx, dc, dev) in enumerate(col_peers):
        rel = {0: 0, 1: 1, 2: 3, 3: 2}[dx]
        csend.append(go(remote(c_ref, cp.at[rel, c], cs.at[n], cr.at[n], dev)))
    cp[0, c] = c_ref[...]

    def left_copy(dx):
        return remote(v_ref.at[0, :, pl.ds(dx * Q, Q), :], lnear.at[OWN - 5, 0:KP], ls.at[dx], lr.at[0], {"gy": dx})

    def leftc_copy(dx):
        return remote(c_ref.at[0], cw.at[OWN], ls.at[NX + dx], lr.at[1], {"gy": dx})

    @pl.when(x == 0)
    def _():
        for dx in (2, 1, 3):
            leftc_copy(dx).start()
        for dx in (2, 1, 3):
            left_copy(dx).start()

    xsend, dsend = {}, {}
    for order in range(2):
        for way, half, dev in ((0, order, xright), (1, 1 - order, xleft)):
            rows = pl.ds(2 * half, 2)
            xsend[way, half] = go(remote(v_ref.at[rows], pall.at[1 + way, c, rows],
                                         xs.at[way, half], xr.at[way, half], {"gy": dev}))
    for half in range(2):
        rows = pl.ds(2 * half, 2)
        dsend[0, half] = go(remote(v_ref.at[rows], v_ref.at[rows], ds.at[0, half], dr.at[0, half], sib))
    for p in range(NZ):
        slot(p)[KP] = jnp.zeros((Q, T), BF16)

    @pl.when(x == 0)
    def _():
        lnear[OWN - 5, 0:KP] = pall[0, c, 0, :, 0:Q, :]
        cw[OWN] = c_ref[0]

    @pl.when(x != 0)
    def _():
        leftc_copy(0).wait_recv()

    ring = [(off, OFFSETS.index(off), at_z(z - off, c)) for off in (1, -1, -2, 2, 3, -3, 4)]
    wcsend = {p: go(remote(cw.at[OWN], cw.at[p], ws.at[1, p], wr.at[1, p], dev)) for off, p, dev in ring}

    @pl.when(x != 0)
    def _():
        left_copy(0).wait_recv()

    wsend = {p: go(remote(slot(OWN).at[0:KP], slot(p).at[0:KP], ws.at[0, p], wr.at[0, p], dev)) for off, p, dev in ring}
    for copy in csend:
        copy.wait_recv()
    cols_copy = pltpu.make_async_copy(cp, cps, loc.at[0])
    cols_copy.start()
    lane = lax.broadcasted_iota(jnp.int32, (1, T), 1)

    def windows(first, last):
        for p in range(first, last):
            if p != OWN:
                wcsend[p].wait_recv()
            row = cw[p]
            found = jnp.full((1, T), KP, jnp.int32)
            for k in range(KP):
                found = jnp.where(jnp.broadcast_to(row[:, k : k + 1], (1, T)) == lane, k, found)
            mapv[p] = found
        some = pl.ds(first, last - first)
        copy = pltpu.make_async_copy(mapv.at[some], maps.at[some], loc.at[1])
        copy.start()
        for p in range(first, last):
            if p != OWN:
                wsend[p].wait_recv()
        copy.wait()

    direct = []
    R, L, OPP = {"gz": yright}, {"gz": yleft}, {"gz": yopp}

    def squares(jobs):
        def body(n, carry):
            block, r = n // 2, lax.rem(n, 2)
            for u, r0, size in jobs:
                rel, row = u // 2, 2 * (u % 2) + r
                wide = []
                for k in range(KP):
                    col = cps[rel, block, row, 0, k]
                    wide.append(jnp.concatenate(
                        [slot(p)[maps[p, 0, col]] for p in range(r0 // Q, (r0 + size) // Q)], axis=0))
                total = None
                for k in range(0, KP, 2):
                    lhs = jnp.concatenate(wide[k : k + 2], axis=1)
                    rhs = jnp.concatenate([pall[rel, block, row, k], pall[rel, block, row, k + 1]], axis=1)
                    prod = nt_dot(lhs, rhs)
                    total = prod if total is None else total + prod
                sb[u, n, r0 : r0 + size] = total.astype(BF16)
            return carry

        lax.fori_loop(0, 4, body, 0)
        for job in jobs:
            for m in range(3) if job in direct else range(4):
                go(message(job, m))


    def message(job, m):
        u, r0, size = job
        n, h = u * 2 + (1 if r0 else 0), size // 2
        top, bottom = pl.ds(r0, h), pl.ds(r0 + h, h)
        part = pl.ds(r0 // 2, h)
        if job in direct:
            dev = (R, L, OPP)[m % 3]
            if m < 3:
                src, dst = sb.at[u, (yright, yleft, yopp)[m], pl.ds(r0, size)], dparts.at[u % 2, m]
            else:
                src = dst = sfin.at[u, y, pl.ds(r0, size)]
        elif m == 0:
            src, dst, dev = sb.at[u, yopp, bottom], relay.at[u, 0, part], R
        elif m == 1:
            src, dst, dev = sb.at[u, yopp, top], relay.at[u, 1, part], L
        elif m == 2:
            src, dst, dev = sb.at[u, yright, top], parts.at[u, 0, part], R
        elif m == 3:
            src, dst, dev = sb.at[u, yleft, bottom], parts.at[u, 1, part], L
        elif m == 4:
            src, dst, dev = fwd.at[u, 0, part], parts.at[u, 2, part], R
        elif m == 5:
            src, dst, dev = fwd.at[u, 1, part], parts.at[u, 3, part], L
        elif m < 10:
            src = dst = sfin.at[u, y, top if m in (6, 8) else bottom]
            dev = R if m < 8 else L
        elif m == 10:
            src = dst = sfin.at[u, yleft, top]
            dev = R
        else:
            src = dst = sfin.at[u, yright, bottom]
            dev = L
        return remote(src, dst, ys.at[n, m], yr.at[n, m], dev)

    def send_relay(job):
        u, r0, size = job
        q, h = r0 // 2, size // 2
        message(job, 0).wait_recv()
        fwd[u, 0, q : q + h] = (sb[u, yright, r0 + h : r0 + size].astype(F32) + relay[u, 0, q : q + h].astype(F32)).astype(BF16)
        go(message(job, 4))
        message(job, 1).wait_recv()
        fwd[u, 1, q : q + h] = (sb[u, yleft, r0 : r0 + h].astype(F32) + relay[u, 1, q : q + h].astype(F32)).astype(BF16)
        go(message(job, 5))

    def send_sum(job):
        u, r0, size = job
        q, h = r0 // 2, size // 2
        message(job, 2).wait_recv()
        message(job, 5).wait_recv()
        sfin[u, y, r0 : r0 + h] = (
            sb[u, y, r0 : r0 + h].astype(F32) + parts[u, 0, q : q + h].astype(F32) + parts[u, 3, q : q + h].astype(F32)).astype(BF16)
        go(message(job, 6))
        go(message(job, 8))
        message(job, 3).wait_recv()
        message(job, 4).wait_recv()
        sfin[u, y, r0 + h : r0 + size] = (
            sb[u, y, r0 + h : r0 + size].astype(F32) + parts[u, 1, q : q + h].astype(F32) + parts[u, 2, q : q + h].astype(F32)).astype(BF16)
        go(message(job, 9))
        go(message(job, 7))

    def send_sum_direct(job):
        u, r0, size = job
        total = sb[u, y, r0 : r0 + size].astype(F32)
        for m in range(3):
            message(job, m).wait_recv()
            total = total + dparts[u % 2, m].astype(F32)
        sfin[u, y, r0 : r0 + size] = total.astype(BF16)
        for m in range(3, 6):
            go(message(job, m))

    def send_forward(job):
        message(job, 6).wait_recv()
        go(message(job, 10))
        message(job, 9).wait_recv()
        go(message(job, 11))

    def products(jobs):
        for job in jobs:
            for m in (3, 4, 5) if job in direct else (7, 8, 10, 11):
                message(job, m).wait_recv()

        def body(n, carry):
            block, r = n // 2, lax.rem(n, 2)
            for u, r0, size in jobs:
                rel, row = u // 2, 2 * (u % 2) + r
                wide = jnp.concatenate([pall[rel, block, row, k] for k in range(KP)], axis=1)
                both = jnp.dot(sfin[u, n, r0 : r0 + size], wide, preferred_element_type=F32)
                at = ((rel * 2 + block) * RB + row) * KP
                for k in range(KP):
                    prods[at + k, r0 : r0 + size] = both[:, k * T : (k + 1) * T]
            return carry

        lax.fori_loop(0, 4, body, 0)

    def arrive(rel, half):
        rows = pl.ds(2 * half, 2)
        dsend[rel, half] = go(remote(pall.at[rel, c, rows], pall.at[rel, c, rows],
                                     ds.at[rel, half], dr.at[rel, half], sib))

    def each(what, jobs):
        for job in jobs:
            what(job)

    def both_cores(units):
        for key in units:
            dsend[key].wait_recv()

    def jobs_of(units, r0, size):
        return [(rel * 2 + half, r0, size) for rel, half in units]

    O, A, B, C = ((0, 0), (0, 1)), ((1, 0), (2, 1)), ((1, 1), (2, 0)), ((3, 0), (3, 1))
    ofar, onear = jobs_of(O, 0, ROWS - THREE), jobs_of(O, ROWS - THREE, THREE)
    afar, anear = jobs_of(A, 0, ROWS - THREE), jobs_of(A, ROWS - THREE, THREE)
    bfar, brest = jobs_of(B, 0, THREE), jobs_of(B, THREE, ROWS - THREE)
    cfar, crest = jobs_of(C, 0, THREE), jobs_of(C, THREE, ROWS - THREE)
    direct.extend(cfar)
    cols_copy.wait()
    windows(5, 8)
    both_cores(O)
    squares(onear)
    rows = pl.ds(0, 2)
    xsend[0, 0].wait_recv()
    xsend[2, 0] = go(remote(pall.at[1, c, rows], pall.at[3, c, rows], xs.at[2, 0], xr.at[2, 0], {"gy": xright}))
    arrive(1, 0)
    rows = pl.ds(2, 2)
    xsend[1, 1].wait_recv()
    xsend[2, 1] = go(remote(pall.at[2, c, rows], pall.at[3, c, rows], xs.at[2, 1], xr.at[2, 1], {"gy": xleft}))
    arrive(2, 1)
    each(send_relay, onear)
    both_cores(A)
    squares(anear)
    windows(0, 5)
    squares(ofar)
    each(send_sum, onear)
    squares(afar)
    each(send_relay, anear)
    each(send_relay, ofar)
    xsend[0, 1].wait_recv()
    arrive(1, 1)
    xsend[1, 0].wait_recv()
    arrive(2, 0)
    each(send_forward, onear)
    each(send_sum, anear)
    both_cores(B)
    squares(bfar)
    each(send_relay, afar)
    each(send_sum, ofar)
    squares(brest)
    each(send_forward, anear)
    each(send_relay, bfar)
    each(send_sum, afar)
    each(send_forward, ofar)
    xsend[2, 0].wait_recv()
    arrive(3, 0)
    xsend[2, 1].wait_recv()
    arrive(3, 1)
    each(send_sum, bfar)
    both_cores(C)
    squares(cfar)
    squares(crest)
    each(send_forward, afar)
    each(send_relay, brest)
    each(send_forward, bfar)
    sort_tiles(cp, colv, prev, ordv)
    order_copy = pltpu.make_async_copy(ordv, ords, loc.at[0])
    order_copy.start()
    products(ofar)
    each(send_sum_direct, cfar)
    each(send_sum, brest)
    products(afar)
    each(send_relay, crest)
    order_copy.wait()
    products(bfar)

    zdevs = (at_z(z + 1, c), at_z(z - 1, c))
    ahead = lax.rem(y - x + NX, NX)
    here = jnp.where(ahead == 0, 0, jnp.where(ahead == 3, 1, jnp.where(ahead == 1, 2, 3)))

    def scan(way, p):
        rows = slice(p * Q, p * Q + Q)
        run = jnp.zeros((Q, T), F32)
        for part in range(2):
            def body(n, run, part=part):
                for m in range(8):
                    t = n * 8 + m
                    code = ords[part, 0, t]
                    tile = prods[code // 2, rows]
                    run = tile + run * lax.rem(code, 2).astype(F32)
                    sums[way, part * T + t] = run
                return run

            run = lax.fori_loop(0, 16 if part == 0 else TILES // 8 - 16, body, run)
        for n in range(2 * RB):
            last = ords[2, 0, 8 * z + n]
            mine = sfin[here * 2 + n % 4 // 2, n // 4 * 2 + n % 2, rows].astype(F32)
            sums[way, TILES + 1 + n] = sums[way, last] - 1.5 * mine

    def result_tile(way, j):
        own = j - 8 * z
        inside = jnp.logical_and(own >= 0, own < 8)
        return -2.0 * sums[way, jnp.where(inside, TILES + 1 + own, ords[2, 0, j])]

    def zcopy(way, hop, sub):
        return remote(sbuf.at[way, hop % 2, sub], rbuf.at[way, hop, sub],
                      zs.at[way, hop, sub], zr.at[way, hop, sub], zdevs[way])

    def emit(way, hop, sub, have, again=False):
        if again:
            zcopy(way, hop - 2, sub).wait_send()
        if have:
            zcopy(way, hop - 1, sub).wait_recv()
        for t in range(PER):
            tile = result_tile(0 if hop == 0 else way, sub * PER + t)
            if have:
                tile = tile + rbuf[way, hop - 1, sub, t].astype(F32)
            sbuf[way, hop % 2, sub, t] = tile.astype(BF16)
        zcopy(way, hop, sub).start()

    for way in range(2):
        sums[way, TILES] = jnp.zeros((Q, T), F32)
    hs = SUBS // 2
    products(cfar)
    scan(0, 0)

    def hop0(n, carry):
        emit(0, 0, n, False)
        emit(1, 0, n + hs, False)
        return carry

    lax.fori_loop(0, hs, hop0, 0)
    for hop in range(1, 4):
        if hop == 1:
            each(send_forward, brest)
            each(send_sum, crest)
        if hop == 2:
            products(anear)
            products(brest)
            products(crest)
        scan(0, 2 * hop - 1)
        scan(1, 2 * hop)
        if hop == 1:
            products(onear)
            each(send_forward, crest)

        def fresh(n, carry, hop=hop):
            emit(0, hop, n + hs, hop > 1, hop == 3)
            emit(1, hop, n, hop > 1, hop == 3)
            return carry

        def relayed(n, carry, hop=hop):
            emit(0, hop, n, True, hop > 1)
            emit(1, hop, n + hs, True, hop > 1)
            return carry

        lax.fori_loop(0, hs, fresh, 0)
        lax.fori_loop(0, hs, relayed, 0)
    scan(0, OWN)
    for n in range(SUBS):
        sub = n // 2 + hs * (n % 2)
        for way in range(2):
            zcopy(way, 3, sub).wait_recv()
        for t in range(PER):
            j = sub * PER + t
            tile = result_tile(0, j) + rbuf[0, 3, sub, t].astype(F32) + rbuf[1, 3, sub, t].astype(F32)
            o_ref[:, j * T : (j + 1) * T] = tile

    @pl.when(x == 0)
    def _():
        for dx in range(1, NX):
            left_copy(dx).wait_send()
            leftc_copy(dx).wait_send()

    def drain(n, carry):
        for way in range(2):
            for hop in range(2, 4):
                zcopy(way, hop, n).wait_send()
        return carry

    lax.fori_loop(0, SUBS, drain, 0)

    for copy in started:
        copy.wait_send()


def local(block_values, block_cols):
    vmem, sem = pltpu.VMEM, pltpu.SemaphoreType.DMA
    return pl.pallas_call(
        step,
        out_shape=jax.ShapeDtypeStruct((Q, 64 * T), F32),
        in_specs=[pl.BlockSpec(memory_space=pltpu.HBM), pl.BlockSpec(memory_space=pltpu.VMEM)],
        out_specs=pl.BlockSpec(memory_space=pltpu.VMEM),
        scratch_shapes=[
            vmem((RB, 1, T), jnp.int32),
            vmem((NX, 2, RB, KP, T, T), BF16),
            vmem((5, KP + 1, Q, T), BF16),
            vmem((3, KP + 1, Q, T), BF16),
            vmem((NZ, 1, T), jnp.int32),
            vmem((NX, 2, RB, 1, T), jnp.int32),
            vmem((NZ, 1, T), jnp.int32),
            pltpu.SMEM((NZ, 1, T), jnp.int32),
            pltpu.SMEM((NX, 2, RB, 1, T), jnp.int32),
            vmem((8, 4, ROWS, T), BF16),
            vmem((8, 2, HALF, T), BF16),
            vmem((8, 4, HALF, T), BF16),
            vmem((2, 3, THREE, T), BF16),
            vmem((8, 2, HALF, T), BF16),
            vmem((8, 4, ROWS, T), BF16),
            vmem((2 * NX * RB, T), jnp.int32),
            vmem((2 * NX * RB, T), jnp.int32),
            vmem((3, 1, T), jnp.int32),
            pltpu.SMEM((3, 1, T), jnp.int32),
            vmem((TILES, ROWS, T), F32),
            vmem((2, TILES + 9, Q, T), F32),
            vmem((2, 4, SUBS, PER, Q, T), BF16),
            vmem((2, 2, SUBS, PER, Q, T), BF16),
            sem((3, 2)), sem((3, 2)), sem((4, 2)), sem((4, 2)),
            sem((7,)), sem((7,)), sem((8,)), sem((2,)),
            sem((2, NZ)), sem((2, NZ)), sem((16, 12)), sem((16, 12)),
            sem((3,)), sem((2, 4, SUBS)), sem((2, 4, SUBS)),
        ],
        compiler_params=pltpu.CompilerParams(
            collective_id=0, has_side_effects=True, vmem_limit_bytes=VMEM_MIB << 20),
        name="step",
    )(block_values.reshape(RB, KP, T, T), block_cols)


def solution(mesh):
    in_specs = (P("gy", "gx", "gz", None, None, None), P("gy", "gx", "gz", None))
    return jax.shard_map(local, mesh=mesh, in_specs=in_specs, out_specs=P(("gx", "gy"), "gz"), check_vma=False)
```

```python
import functools

import jax
import jax.numpy as jnp
from jax import lax
from jax.experimental import pallas as pl
from jax.experimental.pallas import tpu as pltpu
from jax.sharding import PartitionSpec as P

MESH = pl.DeviceIdType.MESH
F32, BF16 = jnp.float32, jnp.bfloat16
NZ, NX, NY = 8, 4, 4
RB, KP, T = 4, 6, 128
Q = T // NX
ROWS = NZ * Q
HALF = ROWS // 2
OFFSETS = (4, 3, -3, 2, -2, 1, -1, 0)
OWN = 7
THREE = 3 * Q
VMEM_MIB = 51
TILES = NX * 2 * RB * KP
SUBS = 8
PER = 64 // SUBS


def where_am_i():
    g = lax.axis_index("gx")
    return g // 2, lax.rem(g, 2), lax.axis_index("gy"), lax.axis_index("gz")


def at_z(z, c):
    return {"gx": lax.rem(z + 2 * NZ, NZ) * 2 + c}


def greet(devices):
    barrier = pltpu.get_barrier_semaphore()
    for device in devices:
        pl.semaphore_signal(barrier, inc=1, device_id=device, device_id_type=MESH)
    pl.semaphore_wait(barrier, len(devices))


def nt_dot(a, b):
    return lax.dot_general(a, b, (((1,), (1,)), ((), ())), preferred_element_type=F32)


def sort_tiles(cp, colv, prev, ordv):
    for n in range(2 * NX * RB):
        colv[n : n + 1, :] = cp[n // 8, n // 4 % 2, n % 4]
    count = 2 * NX * RB
    cols = colv[...]
    lanes = lax.broadcasted_iota(jnp.int32, (count, T), 1)
    hits = [jnp.broadcast_to(cols[:, k : k + 1], (count, T)) == lanes for k in range(KP)]
    listed = jnp.zeros((count, T), jnp.int32)
    for hit in hits:
        listed = listed + jnp.where(hit, 1, 0)
    run = jnp.zeros((1, T), jnp.int32)
    for n in range(count):
        prev[n : n + 1, :] = run
        run = run + listed[n : n + 1, :]
    lane = lax.broadcasted_iota(jnp.int32, (1, T), 1)
    upto = run
    for shift in (1, 2, 4, 8, 16, 32, 64):
        upto = upto + jnp.where(lane >= shift, pltpu.roll(upto, shift, 1), 0)
    before = prev[...]
    place = (jnp.broadcast_to(upto - run, (count, T)) + before) * 2 + jnp.where(before > 0, 1, 0)
    ordv[2] = jnp.where(run > 0, upto - 1, TILES)
    tile = lax.broadcasted_iota(jnp.int32, (count, T), 0) * KP
    picked = [jnp.zeros((count, T), jnp.int32) for part in range(2)]
    for k, hit in enumerate(hits):
        mine = jnp.sum(jnp.where(hit, place, 0), axis=1, keepdims=True)
        mine = jnp.broadcast_to(mine, (count, T))
        code = (tile + k) * 2 + jnp.where(lax.rem(mine, 2) == 1, 1, 0)
        for part in range(2):
            picked[part] = jnp.where(mine // 2 == lanes + part * T, code, picked[part])
    for part in range(2):
        ordv[part] = jnp.sum(picked[part], axis=0, keepdims=True)


def step(v_hbm, c_in, o_ref,
         c_ref, pall, lfar, lnear, cw, cp, mapv, maps, cps, sb, relay, parts, dparts, fwd, sfin,
         colv, prev, ordv, ords, prods, sums, rbuf, sbuf,
         xs, xr, ds, dr, cs, cr, ls, lr, ws, wr, ys, yr, loc, zs, zr):
    z, c, x, y = where_am_i()
    xright, xleft = lax.rem(x + 1, NX), lax.rem(x + 3, NX)
    yright, yleft, yopp = lax.rem(y + 1, NY), lax.rem(y + 3, NY), lax.rem(y + 2, NY)
    sib = {"gx": z * 2 + 1 - c}

    def remote(src, dst, ssem, rsem, device):
        return pltpu.make_async_remote_copy(
            src_ref=src, dst_ref=dst, send_sem=ssem, recv_sem=rsem,
            device_id=device, device_id_type=MESH)

    v_ref = pall.at[0, c]
    fetch = pltpu.make_async_copy(v_hbm, v_ref, loc.at[2])
    fetch.start()
    for r in range(RB):
        c_ref[r] = jnp.zeros((1, T), jnp.int32)
        c_ref[r, :, 0:KP] = c_in[0, r]

    col_peers = []
    for dx in range(NX):
        for dc in range(2):
            if dx or dc:
                col_peers.append((dx, dc, {"gx": z * 2 + lax.rem(c + dc, 2), "gy": lax.rem(x + dx, NX)}))
    greet([p[2] for p in col_peers] + [at_z(z + d, c) for d in range(1, NZ)]
          + [{"gz": yright}, {"gz": yleft}, {"gz": yopp}])
    fetch.wait()
    started = []

    def slot(p):
        return lfar.at[p] if p < 5 else lnear.at[p - 5]

    def go(copy):
        copy.start()
        started.append(copy)
        return copy

    csend = []
    for n, (dx, dc, dev) in enumerate(col_peers):
        rel = {0: 0, 1: 1, 2: 3, 3: 2}[dx]
        csend.append(go(remote(c_ref, cp.at[rel, c], cs.at[n], cr.at[n], dev)))
    cp[0, c] = c_ref[...]

    def left_copy(dx):
        return remote(v_ref.at[0, :, pl.ds(dx * Q, Q), :], lnear.at[OWN - 5, 0:KP], ls.at[dx], lr.at[0], {"gy": dx})

    def leftc_copy(dx):
        return remote(c_ref.at[0], cw.at[OWN], ls.at[NX + dx], lr.at[1], {"gy": dx})

    @pl.when(x == 0)
    def _():
        for dx in (2, 1, 3):
            leftc_copy(dx).start()
        for dx in (2, 1, 3):
            left_copy(dx).start()

    xsend, dsend = {}, {}
    for order in range(2):
        for way, half, dev in ((0, order, xright), (1, 1 - order, xleft)):
            rows = pl.ds(2 * half, 2)
            xsend[way, half] = go(remote(v_ref.at[rows], pall.at[1 + way, c, rows],
                                         xs.at[way, half], xr.at[way, half], {"gy": dev}))
    for half in range(2):
        rows = pl.ds(2 * half, 2)
        dsend[0, half] = go(remote(v_ref.at[rows], v_ref.at[rows], ds.at[0, half], dr.at[0, half], sib))
    for p in range(NZ):
        slot(p)[KP] = jnp.zeros((Q, T), BF16)

    @pl.when(x == 0)
    def _():
        lnear[OWN - 5, 0:KP] = pall[0, c, 0, :, 0:Q, :]
        cw[OWN] = c_ref[0]

    @pl.when(x != 0)
    def _():
        leftc_copy(0).wait_recv()

    ring = [(off, OFFSETS.index(off), at_z(z - off, c)) for off in (1, -1, -2, 2, 3, -3, 4)]
    wcsend = {p: go(remote(cw.at[OWN], cw.at[p], ws.at[1, p], wr.at[1, p], dev)) for off, p, dev in ring}

    @pl.when(x != 0)
    def _():
        left_copy(0).wait_recv()

    wsend = {p: go(remote(slot(OWN).at[0:KP], slot(p).at[0:KP], ws.at[0, p], wr.at[0, p], dev)) for off, p, dev in ring}
    for copy in csend:
        copy.wait_recv()
    cols_copy = pltpu.make_async_copy(cp, cps, loc.at[0])
    cols_copy.start()
    lane = lax.broadcasted_iota(jnp.int32, (1, T), 1)

    def slots_of(first, last, sem):
        for p in range(first, last):
            if p != OWN:
                wcsend[p].wait_recv()
            row = cw[p]
            found = jnp.full((1, T), KP, jnp.int32)
            for k in range(KP):
                found = jnp.where(jnp.broadcast_to(row[:, k : k + 1], (1, T)) == lane, k, found)
            mapv[p] = found
        some = pl.ds(first, last - first)
        copy = pltpu.make_async_copy(mapv.at[some], maps.at[some], sem)
        copy.start()
        return copy

    def windows(first, last):
        for p in range(first, last):
            if p != OWN:
                wsend[p].wait_recv()

    direct = []
    R, L, OPP = {"gz": yright}, {"gz": yleft}, {"gz": yopp}

    def each(what, jobs):
        for job in jobs:
            what(job)

    def send_parts(job):
        for m in range(3) if job in direct else range(4):
            go(message(job, m))

    def squares(jobs, send=True):
        def body(n, carry):
            block, r = n // 2, lax.rem(n, 2)
            for u, r0, size in jobs:
                rel, row = u // 2, 2 * (u % 2) + r
                wide = []
                for k in range(KP):
                    col = cps[rel, block, row, 0, k]
                    wide.append(jnp.concatenate(
                        [slot(p)[maps[p, 0, col]] for p in range(r0 // Q, (r0 + size) // Q)], axis=0))
                total = None
                for k in range(0, KP, 2):
                    lhs = jnp.concatenate(wide[k : k + 2], axis=1)
                    rhs = jnp.concatenate([pall[rel, block, row, k], pall[rel, block, row, k + 1]], axis=1)
                    prod = nt_dot(lhs, rhs)
                    total = prod if total is None else total + prod
                sb[u, n, r0 : r0 + size] = total.astype(BF16)
            return carry

        lax.fori_loop(0, 4, body, 0)
        if send:
            each(send_parts, jobs)


    def message(job, m):
        u, r0, size = job
        n, h = u * 2 + (1 if r0 else 0), size // 2
        top, bottom = pl.ds(r0, h), pl.ds(r0 + h, h)
        part = pl.ds(r0 // 2, h)
        if job in direct:
            dev = (R, L, OPP)[m % 3]
            if m < 3:
                src, dst = sb.at[u, (yright, yleft, yopp)[m], pl.ds(r0, size)], dparts.at[direct.index(job), m]
            else:
                src = dst = sfin.at[u, y, pl.ds(r0, size)]
        elif m == 0:
            src, dst, dev = sb.at[u, yopp, bottom], relay.at[u, 0, part], R
        elif m == 1:
            src, dst, dev = sb.at[u, yopp, top], relay.at[u, 1, part], L
        elif m == 2:
            src, dst, dev = sb.at[u, yright, top], parts.at[u, 0, part], R
        elif m == 3:
            src, dst, dev = sb.at[u, yleft, bottom], parts.at[u, 1, part], L
        elif m == 4:
            src, dst, dev = fwd.at[u, 0, part], parts.at[u, 2, part], R
        elif m == 5:
            src, dst, dev = fwd.at[u, 1, part], parts.at[u, 3, part], L
        elif m < 10:
            src = dst = sfin.at[u, y, top if m in (6, 8) else bottom]
            dev = R if m < 8 else L
        elif m == 10:
            src = dst = sfin.at[u, yleft, top]
            dev = R
        else:
            src = dst = sfin.at[u, yright, bottom]
            dev = L
        return remote(src, dst, ys.at[n, m], yr.at[n, m], dev)

    def send_relay(job):
        u, r0, size = job
        q, h = r0 // 2, size // 2
        message(job, 0).wait_recv()
        fwd[u, 0, q : q + h] = (sb[u, yright, r0 + h : r0 + size].astype(F32) + relay[u, 0, q : q + h].astype(F32)).astype(BF16)
        go(message(job, 4))
        message(job, 1).wait_recv()
        fwd[u, 1, q : q + h] = (sb[u, yleft, r0 : r0 + h].astype(F32) + relay[u, 1, q : q + h].astype(F32)).astype(BF16)
        go(message(job, 5))

    def send_sum(job):
        u, r0, size = job
        q, h = r0 // 2, size // 2
        message(job, 2).wait_recv()
        message(job, 5).wait_recv()
        sfin[u, y, r0 : r0 + h] = (
            sb[u, y, r0 : r0 + h].astype(F32) + parts[u, 0, q : q + h].astype(F32) + parts[u, 3, q : q + h].astype(F32)).astype(BF16)
        go(message(job, 6))
        go(message(job, 8))
        message(job, 3).wait_recv()
        message(job, 4).wait_recv()
        sfin[u, y, r0 + h : r0 + size] = (
            sb[u, y, r0 + h : r0 + size].astype(F32) + parts[u, 1, q : q + h].astype(F32) + parts[u, 2, q : q + h].astype(F32)).astype(BF16)
        go(message(job, 9))
        go(message(job, 7))

    def send_sum_direct(job):
        u, r0, size = job
        total = sb[u, y, r0 : r0 + size].astype(F32)
        for m in range(3):
            message(job, m).wait_recv()
            total = total + dparts[direct.index(job), m].astype(F32)
        sfin[u, y, r0 : r0 + size] = total.astype(BF16)
        for m in range(3, 6):
            go(message(job, m))

    def send_forward(job):
        message(job, 6).wait_recv()
        go(message(job, 10))
        message(job, 9).wait_recv()
        go(message(job, 11))

    def products(jobs):
        for job in jobs:
            for m in (3, 4, 5) if job in direct else (7, 8, 10, 11):
                message(job, m).wait_recv()

        def body(n, carry):
            block, r = n // 2, lax.rem(n, 2)
            for u, r0, size in jobs:
                rel, row = u // 2, 2 * (u % 2) + r
                wide = jnp.concatenate([pall[rel, block, row, k] for k in range(KP)], axis=1)
                both = jnp.dot(sfin[u, n, r0 : r0 + size], wide, preferred_element_type=F32)
                at = ((rel * 2 + block) * RB + row) * KP
                for k in range(KP):
                    prods[at + k, r0 : r0 + size] = both[:, k * T : (k + 1) * T]
            return carry

        lax.fori_loop(0, 4, body, 0)

    def arrive(rel, half):
        rows = pl.ds(2 * half, 2)
        dsend[rel, half] = go(remote(pall.at[rel, c, rows], pall.at[rel, c, rows],
                                     ds.at[rel, half], dr.at[rel, half], sib))

    def both_cores(units):
        for key in units:
            dsend[key].wait_recv()

    def jobs_of(units, r0, size):
        return [(rel * 2 + half, r0, size) for rel, half in units]

    O, A, B, C = ((0, 0), (0, 1)), ((1, 0), (2, 1)), ((1, 1), (2, 0)), ((3, 0), (3, 1))
    ofar, onear = jobs_of(O, 0, ROWS - THREE), jobs_of(O, ROWS - THREE, THREE)
    afar, anear = jobs_of(A, 0, ROWS - THREE), jobs_of(A, ROWS - THREE, THREE)
    bfar, brest = jobs_of(B, 0, THREE), jobs_of(B, THREE, ROWS - THREE)
    cfar, crest = jobs_of(C, 0, THREE), jobs_of(C, THREE, ROWS - THREE)
    direct.extend(bfar + cfar)
    cols_copy.wait()
    near_slots = slots_of(5, 8, loc.at[1])
    windows(5, 8)
    near_slots.wait()
    both_cores(O)
    squares(onear)
    far_slots = slots_of(0, 5, loc.at[3])
    sort_tiles(cp, colv, prev, ordv)
    order_copy = pltpu.make_async_copy(ordv, ords, loc.at[0])
    order_copy.start()
    rows = pl.ds(0, 2)
    xsend[0, 0].wait_recv()
    xsend[2, 0] = go(remote(pall.at[1, c, rows], pall.at[3, c, rows], xs.at[2, 0], xr.at[2, 0], {"gy": xright}))
    arrive(1, 0)
    rows = pl.ds(2, 2)
    xsend[1, 1].wait_recv()
    xsend[2, 1] = go(remote(pall.at[2, c, rows], pall.at[3, c, rows], xs.at[2, 1], xr.at[2, 1], {"gy": xleft}))
    arrive(2, 1)
    each(send_relay, onear)
    far_slots.wait()
    both_cores(A)
    squares(anear)
    windows(0, 5)
    squares(ofar)
    each(send_sum, onear)
    squares(afar)
    each(send_relay, anear)
    each(send_relay, ofar)
    xsend[0, 1].wait_recv()
    arrive(1, 1)
    xsend[1, 0].wait_recv()
    arrive(2, 0)
    each(send_relay, afar)
    both_cores(B)
    squares(bfar)
    each(send_sum, ofar)
    each(send_sum, afar)
    xsend[2, 0].wait_recv()
    arrive(3, 0)
    xsend[2, 1].wait_recv()
    arrive(3, 1)
    each(send_sum_direct, bfar)
    both_cores(C)
    squares(cfar)
    each(send_forward, ofar)
    each(send_forward, afar)
    squares(brest, send=False)
    each(send_sum_direct, cfar)
    each(send_parts, brest)
    products(ofar)
    products(bfar)
    squares(crest)
    products(afar)
    order_copy.wait()

    zdevs = (at_z(z + 1, c), at_z(z - 1, c))
    ahead = lax.rem(y - x + NX, NX)
    here = jnp.where(ahead == 0, 0, jnp.where(ahead == 3, 1, jnp.where(ahead == 1, 2, 3)))

    def scan(way, p):
        rows = slice(p * Q, p * Q + Q)
        run = jnp.zeros((Q, T), F32)
        for part in range(2):
            def body(n, run, part=part):
                for m in range(8):
                    t = n * 8 + m
                    code = ords[part, 0, t]
                    tile = prods[code // 2, rows]
                    run = tile + run * lax.rem(code, 2).astype(F32)
                    sums[way, part * T + t] = run
                return run

            run = lax.fori_loop(0, 16 if part == 0 else TILES // 8 - 16, body, run)
        for n in range(2 * RB):
            last = ords[2, 0, 8 * z + n]
            mine = sfin[here * 2 + n % 4 // 2, n // 4 * 2 + n % 2, rows].astype(F32)
            sums[way, TILES + 1 + n] = sums[way, last] - 1.5 * mine

    def result_tile(way, j):
        own = j - 8 * z
        inside = jnp.logical_and(own >= 0, own < 8)
        return -2.0 * sums[way, jnp.where(inside, TILES + 1 + own, ords[2, 0, j])]

    def zcopy(way, hop, sub):
        return remote(sbuf.at[way, hop % 2, sub], rbuf.at[way, hop, sub],
                      zs.at[way, hop, sub], zr.at[way, hop, sub], zdevs[way])

    def emit(way, hop, sub, have, again=False):
        if again:
            zcopy(way, hop - 2, sub).wait_send()
        if have:
            zcopy(way, hop - 1, sub).wait_recv()
        for t in range(PER):
            tile = result_tile(0 if hop == 0 else way, sub * PER + t)
            if have:
                tile = tile + rbuf[way, hop - 1, sub, t].astype(F32)
            sbuf[way, hop % 2, sub, t] = tile.astype(BF16)
        zcopy(way, hop, sub).start()

    for way in range(2):
        sums[way, TILES] = jnp.zeros((Q, T), F32)
    hs = SUBS // 2
    products(cfar)
    scan(0, 0)

    def hop0(n, carry):
        emit(0, 0, n, False)
        emit(1, 0, n + hs, False)
        return carry

    lax.fori_loop(0, hs, hop0, 0)
    for hop in range(1, 4):
        if hop == 1:
            each(send_forward, onear)
            each(send_sum, anear)
            each(send_relay, brest)
            each(send_relay, crest)
        if hop == 2:
            products(brest)
            products(crest)
        scan(0, 2 * hop - 1)
        scan(1, 2 * hop)

        def fresh(n, carry, hop=hop):
            emit(0, hop, n + hs, hop > 1, hop == 3)
            emit(1, hop, n, hop > 1, hop == 3)
            return carry

        def relayed(n, carry, hop=hop):
            emit(0, hop, n, True, hop > 1)
            emit(1, hop, n + hs, True, hop > 1)
            return carry

        lax.fori_loop(0, hs, fresh, 0)
        if hop == 1:
            each(send_sum, brest)
            each(send_sum, crest)
        lax.fori_loop(0, hs // 2, relayed, 0)
        if hop == 1:
            each(send_forward, brest)
            each(send_forward, crest)
            each(send_forward, anear)
        lax.fori_loop(hs // 2, hs, relayed, 0)
        if hop == 1:
            products(onear)
            products(anear)
    scan(0, OWN)
    for n in range(SUBS):
        sub = n // 2 + hs * (n % 2)
        for way in range(2):
            zcopy(way, 3, sub).wait_recv()
        for t in range(PER):
            j = sub * PER + t
            tile = result_tile(0, j) + rbuf[0, 3, sub, t].astype(F32) + rbuf[1, 3, sub, t].astype(F32)
            o_ref[:, j * T : (j + 1) * T] = tile

    @pl.when(x == 0)
    def _():
        for dx in range(1, NX):
            left_copy(dx).wait_send()
            leftc_copy(dx).wait_send()

    def drain(n, carry):
        for way in range(2):
            for hop in range(2, 4):
                zcopy(way, hop, n).wait_send()
        return carry

    lax.fori_loop(0, SUBS, drain, 0)

    for copy in started:
        copy.wait_send()


def local(block_values, block_cols):
    vmem, sem = pltpu.VMEM, pltpu.SemaphoreType.DMA
    return pl.pallas_call(
        step,
        out_shape=jax.ShapeDtypeStruct((Q, 64 * T), F32),
        in_specs=[pl.BlockSpec(memory_space=pltpu.HBM), pl.BlockSpec(memory_space=pltpu.VMEM)],
        out_specs=pl.BlockSpec(memory_space=pltpu.VMEM),
        scratch_shapes=[
            vmem((RB, 1, T), jnp.int32),
            vmem((NX, 2, RB, KP, T, T), BF16),
            vmem((5, KP + 1, Q, T), BF16),
            vmem((3, KP + 1, Q, T), BF16),
            vmem((NZ, 1, T), jnp.int32),
            vmem((NX, 2, RB, 1, T), jnp.int32),
            vmem((NZ, 1, T), jnp.int32),
            pltpu.SMEM((NZ, 1, T), jnp.int32),
            pltpu.SMEM((NX, 2, RB, 1, T), jnp.int32),
            vmem((8, 4, ROWS, T), BF16),
            vmem((8, 2, HALF, T), BF16),
            vmem((8, 4, HALF, T), BF16),
            vmem((4, 3, THREE, T), BF16),
            vmem((8, 2, HALF, T), BF16),
            vmem((8, 4, ROWS, T), BF16),
            vmem((2 * NX * RB, T), jnp.int32),
            vmem((2 * NX * RB, T), jnp.int32),
            vmem((3, 1, T), jnp.int32),
            pltpu.SMEM((3, 1, T), jnp.int32),
            vmem((TILES, ROWS, T), F32),
            vmem((2, TILES + 9, Q, T), F32),
            vmem((2, 4, SUBS, PER, Q, T), BF16),
            vmem((2, 2, SUBS, PER, Q, T), BF16),
            sem((3, 2)), sem((3, 2)), sem((4, 2)), sem((4, 2)),
            sem((7,)), sem((7,)), sem((8,)), sem((2,)),
            sem((2, NZ)), sem((2, NZ)), sem((16, 12)), sem((16, 12)),
            sem((4,)), sem((2, 4, SUBS)), sem((2, 4, SUBS)),
        ],
        compiler_params=pltpu.CompilerParams(
            collective_id=0, has_side_effects=True, vmem_limit_bytes=VMEM_MIB << 20),
        name="step",
    )(block_values.reshape(RB, KP, T, T), block_cols)


def solution(mesh):
    in_specs = (P("gy", "gx", "gz", None, None, None), P("gy", "gx", "gz", None))
    return jax.shard_map(local, mesh=mesh, in_specs=in_specs, out_specs=P(("gx", "gy"), "gz"), check_vma=False)
```

```python
import functools

import jax
import jax.numpy as jnp
from jax import lax
from jax.experimental import pallas as pl
from jax.experimental.pallas import tpu as pltpu
from jax.sharding import PartitionSpec as P

MESH = pl.DeviceIdType.MESH
F32, BF16 = jnp.float32, jnp.bfloat16
NZ, NX, NY = 8, 4, 4
RB, KP, T = 4, 6, 128
Q = T // NX
ROWS = NZ * Q
HALF = ROWS // 2
OFFSETS = (4, 3, -3, 2, -2, 1, -1, 0)
OWN = 7
THREE = 3 * Q
VMEM_MIB = 51
TILES = NX * 2 * RB * KP
SUBS = 8
PER = 64 // SUBS


def where_am_i():
    g = lax.axis_index("gx")
    return g // 2, lax.rem(g, 2), lax.axis_index("gy"), lax.axis_index("gz")


def at_z(z, c):
    return {"gx": lax.rem(z + 2 * NZ, NZ) * 2 + c}


def greet(devices):
    barrier = pltpu.get_barrier_semaphore()
    for device in devices:
        pl.semaphore_signal(barrier, inc=1, device_id=device, device_id_type=MESH)
    pl.semaphore_wait(barrier, len(devices))


def nt_dot(a, b):
    return lax.dot_general(a, b, (((1,), (1,)), ((), ())), preferred_element_type=F32)


def sort_tiles(cp, colv, prev, ordv):
    for n in range(2 * NX * RB):
        colv[n : n + 1, :] = cp[n // 8, n // 4 % 2, n % 4]
    count = 2 * NX * RB
    cols = colv[...]
    lanes = lax.broadcasted_iota(jnp.int32, (count, T), 1)
    hits = [jnp.broadcast_to(cols[:, k : k + 1], (count, T)) == lanes for k in range(KP)]
    listed = jnp.zeros((count, T), jnp.int32)
    for hit in hits:
        listed = listed + jnp.where(hit, 1, 0)
    run = jnp.zeros((1, T), jnp.int32)
    for n in range(count):
        prev[n : n + 1, :] = run
        run = run + listed[n : n + 1, :]
    lane = lax.broadcasted_iota(jnp.int32, (1, T), 1)
    upto = run
    for shift in (1, 2, 4, 8, 16, 32, 64):
        upto = upto + jnp.where(lane >= shift, pltpu.roll(upto, shift, 1), 0)
    before = prev[...]
    place = (jnp.broadcast_to(upto - run, (count, T)) + before) * 2 + jnp.where(before > 0, 1, 0)
    ordv[2] = jnp.where(run > 0, upto - 1, TILES)
    tile = lax.broadcasted_iota(jnp.int32, (count, T), 0) * KP
    picked = [jnp.zeros((count, T), jnp.int32) for part in range(2)]
    for k, hit in enumerate(hits):
        mine = jnp.sum(jnp.where(hit, place, 0), axis=1, keepdims=True)
        mine = jnp.broadcast_to(mine, (count, T))
        code = (tile + k) * 2 + jnp.where(lax.rem(mine, 2) == 1, 1, 0)
        for part in range(2):
            picked[part] = jnp.where(mine // 2 == lanes + part * T, code, picked[part])
    for part in range(2):
        ordv[part] = jnp.sum(picked[part], axis=0, keepdims=True)


def step(v_hbm, c_in, o_ref,
         c_ref, pall, lfar, lnear, cw, cp, mapv, maps, cps, sb, relay, parts, dparts, fwd, sfin,
         colv, prev, ordv, ords, prods, sums, rbuf, sbuf,
         xs, xr, ds, dr, cs, cr, ls, lr, ws, wr, ys, yr, loc, zs, zr):
    z, c, x, y = where_am_i()
    xright, xleft = lax.rem(x + 1, NX), lax.rem(x + 3, NX)
    yright, yleft, yopp = lax.rem(y + 1, NY), lax.rem(y + 3, NY), lax.rem(y + 2, NY)
    sib = {"gx": z * 2 + 1 - c}

    def remote(src, dst, ssem, rsem, device):
        return pltpu.make_async_remote_copy(
            src_ref=src, dst_ref=dst, send_sem=ssem, recv_sem=rsem,
            device_id=device, device_id_type=MESH)

    v_ref = pall.at[0, c]
    fetch = pltpu.make_async_copy(v_hbm, v_ref, loc.at[2])
    fetch.start()
    for r in range(RB):
        c_ref[r] = jnp.zeros((1, T), jnp.int32)
        c_ref[r, :, 0:KP] = c_in[0, r]

    col_peers = []
    for dx in range(NX):
        for dc in range(2):
            if dx or dc:
                col_peers.append((dx, dc, {"gx": z * 2 + lax.rem(c + dc, 2), "gy": lax.rem(x + dx, NX)}))
    greet([p[2] for p in col_peers] + [at_z(z + d, c) for d in range(1, NZ)]
          + [{"gz": yright}, {"gz": yleft}, {"gz": yopp}])
    fetch.wait()
    started = []

    def slot(p):
        return lfar.at[p] if p < 5 else lnear.at[p - 5]

    def go(copy):
        copy.start()
        started.append(copy)
        return copy

    csend = []
    for n, (dx, dc, dev) in enumerate(col_peers):
        rel = {0: 0, 1: 1, 2: 3, 3: 2}[dx]
        csend.append(go(remote(c_ref, cp.at[rel, c], cs.at[n], cr.at[n], dev)))
    cp[0, c] = c_ref[...]

    def left_copy(dx):
        return remote(v_ref.at[0, :, pl.ds(dx * Q, Q), :], lnear.at[OWN - 5, 0:KP], ls.at[dx], lr.at[0], {"gy": dx})

    def leftc_copy(dx):
        return remote(c_ref.at[0], cw.at[OWN], ls.at[NX + dx], lr.at[1], {"gy": dx})

    @pl.when(x == 0)
    def _():
        for dx in (2, 1, 3):
            leftc_copy(dx).start()
        for dx in (2, 1, 3):
            left_copy(dx).start()

    xsend, dsend = {}, {}
    for order in range(2):
        for way, half, dev in ((0, order, xright), (1, 1 - order, xleft)):
            rows = pl.ds(2 * half, 2)
            xsend[way, half] = go(remote(v_ref.at[rows], pall.at[1 + way, c, rows],
                                         xs.at[way, half], xr.at[way, half], {"gy": dev}))
    for half in range(2):
        rows = pl.ds(2 * half, 2)
        dsend[0, half] = go(remote(v_ref.at[rows], v_ref.at[rows], ds.at[0, half], dr.at[0, half], sib))
    for p in range(NZ):
        slot(p)[KP] = jnp.zeros((Q, T), BF16)

    @pl.when(x == 0)
    def _():
        lnear[OWN - 5, 0:KP] = pall[0, c, 0, :, 0:Q, :]
        cw[OWN] = c_ref[0]

    @pl.when(x != 0)
    def _():
        leftc_copy(0).wait_recv()

    ring = [(off, OFFSETS.index(off), at_z(z - off, c)) for off in (1, -1, -2, 2, 3, -3, 4)]
    wcsend = {p: go(remote(cw.at[OWN], cw.at[p], ws.at[1, p], wr.at[1, p], dev)) for off, p, dev in ring}

    @pl.when(x != 0)
    def _():
        left_copy(0).wait_recv()

    wsend = {p: go(remote(slot(OWN).at[0:KP], slot(p).at[0:KP], ws.at[0, p], wr.at[0, p], dev)) for off, p, dev in ring}
    for copy in csend:
        copy.wait_recv()
    cols_copy = pltpu.make_async_copy(cp, cps, loc.at[0])
    cols_copy.start()
    lane = lax.broadcasted_iota(jnp.int32, (1, T), 1)

    def slots_of(first, last, sem):
        for p in range(first, last):
            if p != OWN:
                wcsend[p].wait_recv()
            row = cw[p]
            found = jnp.full((1, T), KP, jnp.int32)
            for k in range(KP):
                found = jnp.where(jnp.broadcast_to(row[:, k : k + 1], (1, T)) == lane, k, found)
            mapv[p] = found
        some = pl.ds(first, last - first)
        copy = pltpu.make_async_copy(mapv.at[some], maps.at[some], sem)
        copy.start()
        return copy

    def windows(first, last):
        for p in range(first, last):
            if p != OWN:
                wsend[p].wait_recv()

    direct = []
    R, L, OPP = {"gz": yright}, {"gz": yleft}, {"gz": yopp}

    def each(what, jobs):
        for job in jobs:
            what(job)

    def send_parts(job):
        for m in range(3) if job in direct else range(4):
            go(message(job, m))

    def squares(jobs, send=True):
        def body(n, carry):
            block, r = n // 2, lax.rem(n, 2)
            for u, r0, size in jobs:
                rel, row = u // 2, 2 * (u % 2) + r
                wide = []
                for k in range(KP):
                    col = cps[rel, block, row, 0, k]
                    wide.append(jnp.concatenate(
                        [slot(p)[maps[p, 0, col]] for p in range(r0 // Q, (r0 + size) // Q)], axis=0))
                total = None
                for k in range(0, KP, 2):
                    lhs = jnp.concatenate(wide[k : k + 2], axis=1)
                    rhs = jnp.concatenate([pall[rel, block, row, k], pall[rel, block, row, k + 1]], axis=1)
                    prod = nt_dot(lhs, rhs)
                    total = prod if total is None else total + prod
                sb[u, n, r0 : r0 + size] = total.astype(BF16)
            return carry

        lax.fori_loop(0, 4, body, 0)
        if send:
            each(send_parts, jobs)


    def message(job, m):
        u, r0, size = job
        n, h = u * 2 + (1 if r0 else 0), size // 2
        top, bottom = pl.ds(r0, h), pl.ds(r0 + h, h)
        part = pl.ds(r0 // 2, h)
        if job in direct:
            dev = (R, L, OPP)[m % 3]
            if m < 3:
                src, dst = sb.at[u, (yright, yleft, yopp)[m], pl.ds(r0, size)], dparts.at[direct.index(job), m]
            else:
                src = dst = sfin.at[u, y, pl.ds(r0, size)]
        elif m == 0:
            src, dst, dev = sb.at[u, yopp, bottom], relay.at[u, 0, part], R
        elif m == 1:
            src, dst, dev = sb.at[u, yopp, top], relay.at[u, 1, part], L
        elif m == 2:
            src, dst, dev = sb.at[u, yright, top], parts.at[u, 0, part], R
        elif m == 3:
            src, dst, dev = sb.at[u, yleft, bottom], parts.at[u, 1, part], L
        elif m == 4:
            src, dst, dev = fwd.at[u, 0, part], parts.at[u, 2, part], R
        elif m == 5:
            src, dst, dev = fwd.at[u, 1, part], parts.at[u, 3, part], L
        elif m < 10:
            src = dst = sfin.at[u, y, top if m in (6, 8) else bottom]
            dev = R if m < 8 else L
        elif m == 10:
            src = dst = sfin.at[u, yleft, top]
            dev = R
        else:
            src = dst = sfin.at[u, yright, bottom]
            dev = L
        return remote(src, dst, ys.at[n, m], yr.at[n, m], dev)

    def send_relay(job):
        u, r0, size = job
        q, h = r0 // 2, size // 2
        message(job, 0).wait_recv()
        fwd[u, 0, q : q + h] = (sb[u, yright, r0 + h : r0 + size].astype(F32) + relay[u, 0, q : q + h].astype(F32)).astype(BF16)
        go(message(job, 4))
        message(job, 1).wait_recv()
        fwd[u, 1, q : q + h] = (sb[u, yleft, r0 : r0 + h].astype(F32) + relay[u, 1, q : q + h].astype(F32)).astype(BF16)
        go(message(job, 5))

    def send_sum(job):
        u, r0, size = job
        q, h = r0 // 2, size // 2
        message(job, 2).wait_recv()
        message(job, 5).wait_recv()
        sfin[u, y, r0 : r0 + h] = (
            sb[u, y, r0 : r0 + h].astype(F32) + parts[u, 0, q : q + h].astype(F32) + parts[u, 3, q : q + h].astype(F32)).astype(BF16)
        go(message(job, 6))
        go(message(job, 8))
        message(job, 3).wait_recv()
        message(job, 4).wait_recv()
        sfin[u, y, r0 + h : r0 + size] = (
            sb[u, y, r0 + h : r0 + size].astype(F32) + parts[u, 1, q : q + h].astype(F32) + parts[u, 2, q : q + h].astype(F32)).astype(BF16)
        go(message(job, 9))
        go(message(job, 7))

    def send_sum_direct(job):
        u, r0, size = job
        total = sb[u, y, r0 : r0 + size].astype(F32)
        for m in range(3):
            message(job, m).wait_recv()
            total = total + dparts[direct.index(job), m].astype(F32)
        sfin[u, y, r0 : r0 + size] = total.astype(BF16)
        for m in range(3, 6):
            go(message(job, m))

    def send_forward(job):
        message(job, 6).wait_recv()
        go(message(job, 10))
        message(job, 9).wait_recv()
        go(message(job, 11))

    def products(jobs):
        for job in jobs:
            for m in (3, 4, 5) if job in direct else (7, 8, 10, 11):
                message(job, m).wait_recv()

        def body(n, carry):
            block, r = n // 2, lax.rem(n, 2)
            for u, r0, size in jobs:
                rel, row = u // 2, 2 * (u % 2) + r
                wide = jnp.concatenate([pall[rel, block, row, k] for k in range(KP)], axis=1)
                both = jnp.dot(sfin[u, n, r0 : r0 + size], wide, preferred_element_type=F32)
                at = ((rel * 2 + block) * RB + row) * KP
                for k in range(KP):
                    prods[at + k, r0 : r0 + size] = both[:, k * T : (k + 1) * T]
            return carry

        lax.fori_loop(0, 4, body, 0)

    def arrive(rel, half):
        rows = pl.ds(2 * half, 2)
        dsend[rel, half] = go(remote(pall.at[rel, c, rows], pall.at[rel, c, rows],
                                     ds.at[rel, half], dr.at[rel, half], sib))

    def both_cores(units):
        for key in units:
            dsend[key].wait_recv()

    def jobs_of(units, r0, size):
        return [(rel * 2 + half, r0, size) for rel, half in units]

    O, A, B, C = ((0, 0), (0, 1)), ((1, 0), (2, 1)), ((1, 1), (2, 0)), ((3, 0), (3, 1))
    ofar, onear = jobs_of(O, 0, ROWS - THREE), jobs_of(O, ROWS - THREE, THREE)
    afar, anear = jobs_of(A, 0, ROWS - THREE), jobs_of(A, ROWS - THREE, THREE)
    bfar, brest = jobs_of(B, 0, THREE), jobs_of(B, THREE, ROWS - THREE)
    cfar, crest = jobs_of(C, 0, THREE), jobs_of(C, THREE, ROWS - THREE)
    direct.extend(bfar + cfar)
    cols_copy.wait()
    near_slots = slots_of(5, 8, loc.at[1])
    windows(5, 8)
    near_slots.wait()
    both_cores(O)
    squares(onear)
    far_slots = slots_of(0, 5, loc.at[3])
    sort_tiles(cp, colv, prev, ordv)
    order_copy = pltpu.make_async_copy(ordv, ords, loc.at[0])
    order_copy.start()
    rows = pl.ds(0, 2)
    xsend[0, 0].wait_recv()
    xsend[2, 0] = go(remote(pall.at[1, c, rows], pall.at[3, c, rows], xs.at[2, 0], xr.at[2, 0], {"gy": xright}))
    arrive(1, 0)
    rows = pl.ds(2, 2)
    xsend[1, 1].wait_recv()
    xsend[2, 1] = go(remote(pall.at[2, c, rows], pall.at[3, c, rows], xs.at[2, 1], xr.at[2, 1], {"gy": xleft}))
    arrive(2, 1)
    each(send_relay, onear)
    far_slots.wait()
    both_cores(A)
    squares(anear)
    windows(0, 5)
    squares(ofar)
    each(send_sum, onear)
    squares(afar)
    each(send_relay, anear)
    each(send_relay, ofar)
    xsend[0, 1].wait_recv()
    arrive(1, 1)
    xsend[1, 0].wait_recv()
    arrive(2, 0)
    each(send_relay, afar)
    both_cores(B)
    squares(bfar)
    each(send_sum, ofar)
    each(send_sum, afar)
    xsend[2, 0].wait_recv()
    arrive(3, 0)
    xsend[2, 1].wait_recv()
    arrive(3, 1)
    each(send_sum_direct, bfar)
    both_cores(C)
    squares(cfar)
    each(send_forward, ofar)
    each(send_forward, afar)
    squares(brest, send=False)
    products(bfar)
    each(send_sum_direct, cfar)
    each(send_parts, brest)
    squares(crest)
    products(ofar)
    products(afar)
    order_copy.wait()

    zdevs = (at_z(z + 1, c), at_z(z - 1, c))
    ahead = lax.rem(y - x + NX, NX)
    here = jnp.where(ahead == 0, 0, jnp.where(ahead == 3, 1, jnp.where(ahead == 1, 2, 3)))

    def scan(*windows):
        spans = [slice(p * Q, p * Q + Q) for p in windows]
        runs = tuple(jnp.zeros((Q, T), F32) for p in windows)
        for part in range(2):
            def body(n, runs, part=part):
                for m in range(8):
                    t = n * 8 + m
                    code = ords[part, 0, t]
                    keep = lax.rem(code, 2).astype(F32)
                    runs = tuple(prods[code // 2, rows] + run * keep for rows, run in zip(spans, runs))
                    for way, run in enumerate(runs):
                        sums[way, part * T + t] = run
                return runs

            runs = lax.fori_loop(0, 16 if part == 0 else TILES // 8 - 16, body, runs)
        for n in range(2 * RB):
            last = ords[2, 0, 8 * z + n]
            for way, rows in enumerate(spans):
                mine = sfin[here * 2 + n % 4 // 2, n // 4 * 2 + n % 2, rows].astype(F32)
                sums[way, TILES + 1 + n] = sums[way, last] - 1.5 * mine

    def result_tile(way, j):
        own = j - 8 * z
        inside = jnp.logical_and(own >= 0, own < 8)
        return -2.0 * sums[way, jnp.where(inside, TILES + 1 + own, ords[2, 0, j])]

    def zcopy(way, hop, sub):
        return remote(sbuf.at[way, hop % 2, sub], rbuf.at[way, hop, sub],
                      zs.at[way, hop, sub], zr.at[way, hop, sub], zdevs[way])

    def emit(way, hop, sub, have, again=False):
        if again:
            zcopy(way, hop - 2, sub).wait_send()
        if have:
            zcopy(way, hop - 1, sub).wait_recv()
        for t in range(PER):
            tile = result_tile(0 if hop == 0 else way, sub * PER + t)
            if have:
                tile = tile + rbuf[way, hop - 1, sub, t].astype(F32)
            sbuf[way, hop % 2, sub, t] = tile.astype(BF16)
        zcopy(way, hop, sub).start()

    for way in range(2):
        sums[way, TILES] = jnp.zeros((Q, T), F32)
    hs = SUBS // 2
    products(cfar)
    scan(0)

    def hop0(n, carry):
        emit(0, 0, n, False)
        emit(1, 0, n + hs, False)
        return carry

    lax.fori_loop(0, hs, hop0, 0)
    for hop in range(1, 4):
        if hop == 1:
            each(send_relay, brest)
            each(send_relay, crest)
        if hop == 2:
            products(brest)
            products(crest)
            each(send_forward, onear)
            each(send_sum, anear)
        if hop == 3:
            products(onear)
            products(anear)
        scan(2 * hop - 1, 2 * hop)

        def fresh(n, carry, hop=hop):
            emit(0, hop, n + hs, hop > 1, hop == 3)
            emit(1, hop, n, hop > 1, hop == 3)
            return carry

        def relayed(n, carry, hop=hop):
            emit(0, hop, n, True, hop > 1)
            emit(1, hop, n + hs, True, hop > 1)
            return carry

        lax.fori_loop(0, hs, fresh, 0)
        if hop == 1:
            each(send_sum, brest)
            each(send_sum, crest)
        lax.fori_loop(0, hs // 2, relayed, 0)
        if hop == 1:
            each(send_forward, brest)
            each(send_forward, crest)
        if hop == 2:
            each(send_forward, anear)
        lax.fori_loop(hs // 2, hs, relayed, 0)
    scan(OWN)
    for n in range(SUBS):
        sub = n // 2 + hs * (n % 2)
        for way in range(2):
            zcopy(way, 3, sub).wait_recv()
        for t in range(PER):
            j = sub * PER + t
            tile = result_tile(0, j) + rbuf[0, 3, sub, t].astype(F32) + rbuf[1, 3, sub, t].astype(F32)
            o_ref[:, j * T : (j + 1) * T] = tile

    @pl.when(x == 0)
    def _():
        for dx in range(1, NX):
            left_copy(dx).wait_send()
            leftc_copy(dx).wait_send()

    def drain(n, carry):
        for way in range(2):
            for hop in range(2, 4):
                zcopy(way, hop, n).wait_send()
        return carry

    lax.fori_loop(0, SUBS, drain, 0)

    for copy in started:
        copy.wait_send()


def local(block_values, block_cols):
    vmem, sem = pltpu.VMEM, pltpu.SemaphoreType.DMA
    return pl.pallas_call(
        step,
        out_shape=jax.ShapeDtypeStruct((Q, 64 * T), F32),
        in_specs=[pl.BlockSpec(memory_space=pltpu.HBM), pl.BlockSpec(memory_space=pltpu.VMEM)],
        out_specs=pl.BlockSpec(memory_space=pltpu.VMEM),
        scratch_shapes=[
            vmem((RB, 1, T), jnp.int32),
            vmem((NX, 2, RB, KP, T, T), BF16),
            vmem((5, KP + 1, Q, T), BF16),
            vmem((3, KP + 1, Q, T), BF16),
            vmem((NZ, 1, T), jnp.int32),
            vmem((NX, 2, RB, 1, T), jnp.int32),
            vmem((NZ, 1, T), jnp.int32),
            pltpu.SMEM((NZ, 1, T), jnp.int32),
            pltpu.SMEM((NX, 2, RB, 1, T), jnp.int32),
            vmem((8, 4, ROWS, T), BF16),
            vmem((8, 2, HALF, T), BF16),
            vmem((8, 4, HALF, T), BF16),
            vmem((4, 3, THREE, T), BF16),
            vmem((8, 2, HALF, T), BF16),
            vmem((8, 4, ROWS, T), BF16),
            vmem((2 * NX * RB, T), jnp.int32),
            vmem((2 * NX * RB, T), jnp.int32),
            vmem((3, 1, T), jnp.int32),
            pltpu.SMEM((3, 1, T), jnp.int32),
            vmem((TILES, ROWS, T), F32),
            vmem((2, TILES + 9, Q, T), F32),
            vmem((2, 4, SUBS, PER, Q, T), BF16),
            vmem((2, 2, SUBS, PER, Q, T), BF16),
            sem((3, 2)), sem((3, 2)), sem((4, 2)), sem((4, 2)),
            sem((7,)), sem((7,)), sem((8,)), sem((2,)),
            sem((2, NZ)), sem((2, NZ)), sem((16, 12)), sem((16, 12)),
            sem((4,)), sem((2, 4, SUBS)), sem((2, 4, SUBS)),
        ],
        compiler_params=pltpu.CompilerParams(
            collective_id=0, has_side_effects=True, vmem_limit_bytes=VMEM_MIB << 20),
        name="step",
    )(block_values.reshape(RB, KP, T, T), block_cols)


def solution(mesh):
    in_specs = (P("gy", "gx", "gz", None, None, None), P("gy", "gx", "gz", None))
    return jax.shard_map(local, mesh=mesh, in_specs=in_specs, out_specs=P(("gx", "gy"), "gz"), check_vma=False)
```
